512 devices in a mesh: blk: 32 (over y, z_lo, core), replica: 16 (over z_hi, x).
Axes of the slice: x: 4, y: 4, z: 16 (z_hi: 4, z_lo: 4; z = z_hi * 4 + z_lo), core: 2. Of those that a mesh axis runs over, the one named last changes fastest.
Arguments:
- tokens: bfloat16 [640, 4096], P('blk', 'replica'), may hold values from -6 to 6
- cotangent: bfloat16 [640, 4096], P('blk', 'replica'), may hold values from -6 to 6
- gate_weight: bfloat16 [4096, 28672], P('replica', 'blk'), may hold values from -36 to 36, as said below
- up_weight: bfloat16 [4096, 28672], P('replica', 'blk'), may hold values from -36 to 36, as said below
- down_weight: bfloat16 [28672, 4096], P('blk', 'replica'), may hold values from -72 to 72, as said below
- gate_gain: float32 [28672], P('blk'), may hold values from 0.25 to 1.75
- up_gain: float32 [28672], P('blk'), may hold values from 0.25 to 1.75
- down_gain: float32 [4096], P('replica'), may hold values from 0.25 to 1.75
Outputs:
- grad_tokens: float32 [640, 4096], P('blk', 'replica')
- grad_gate: float32 [4096, 28672], P('replica', 'blk')
- grad_up: float32 [4096, 28672], P('replica', 'blk')
- grad_down: float32 [28672, 4096], P('blk', 'replica')
- grad_gate_gain: float32 [28672], P('blk')
- grad_up_gain: float32 [28672], P('blk')
- grad_down_gain: float32 [4096], P('replica')
The draws below stay inside these ranges and needn't reach their ends.
Inputs may be any that keep to these rules, and one draw needn't show every extreme that they name: `gate_weight`: real-valued raw weights. `up_weight`: real-valued raw weights. `down_weight`: real-valued raw weights.
All inputs are finite; a program needn't handle non-finite values.
Results may differ from the reference program's by a relative error of at most 0.033.
Values may be sent and summed in bfloat16 or wider, within the bound.
No kernel may reach another device: no remote copies, remote signals or barrier semaphores. Data moves between devices by JAX's collectives and lax.ppermute only.
A program may use at most 64 MiB of HBM per device.

```python
import jax
import jax.numpy as jnp
from jax import lax

D = 4096
FF = 28672
TOKENS = 640
N_REPLICA = 16


def rising_rows(key):
    position = jnp.arange(D, dtype=jnp.float32) / max(D - 1, 1)
    rows = jnp.exp(jnp.log(6.0) * position)
    entries = jnp.clip(jax.random.normal(jax.random.fold_in(key, 13), (D, FF), jnp.float32), -6.0, 6.0)
    value = entries * rows[:, None]
    return jnp.clip(value, -36.0, 36.0).astype(jnp.bfloat16)


def draw_gate_weight(key, part):
    return rising_rows(jax.random.fold_in(key, 101))


def draw_up_weight(key, part):
    return rising_rows(jax.random.fold_in(key, 202))


def draw_down_weight(key, part):
    base = jax.random.fold_in(key, 303)
    position = jnp.arange(FF, dtype=jnp.float32) / max(FF - 1, 1)
    offset = jax.random.uniform(jax.random.fold_in(base, 21), (D,), jnp.float32, 0.5, 1.5)
    rows = jnp.exp(jnp.log(6.0) * position)
    entries = jnp.clip(jax.random.normal(jax.random.fold_in(base, 23), (FF, D), jnp.float32), -6.0, 6.0)
    value = (entries + offset[None, :]) * rows[:, None]
    return jnp.clip(value, -72.0, 72.0).astype(jnp.bfloat16)


def block_levels(own_key, dims, pieces, low, high):
    def one(axis_at, shards_of):
        draws = jax.random.uniform(jax.random.fold_in(jax.random.fold_in(own_key, 6), axis_at), (shards_of,), jnp.float32, low / len(pieces), high / len(pieces))
        return jnp.repeat(jnp.exp(draws), dims[axis_at] // shards_of).reshape((-1,) + (1,) * (len(dims) - axis_at - 1))

    factor_of = one(*pieces[0])
    for cut in pieces[1:]:
        factor_of = factor_of * one(*cut)
    return factor_of


def gaussian(stream_key, shape, width, limit, cuts=(), kind=jnp.bfloat16):
    values = jax.random.normal(stream_key, shape, jnp.float32) * width
    if len(cuts) > 0:
        values = block_levels(stream_key, shape, cuts, -0.22, 0.18) * values
    return jnp.clip(values, min=-limit, max=limit).astype(kind)


def setup_inputs(seed: int = 0) -> dict:
    seeds = jax.random.split(jax.random.key(seed), 9)
    return {
        "tokens": gaussian(seeds[0], (TOKENS, D), 1.0, 6.0, ((0, 32), (1, 16))),
        "cotangent": gaussian(seeds[1], (TOKENS, D), 1.0, 6.0, ((0, 32), (1, 16))),
        "gate_weight": draw_gate_weight(jax.random.fold_in(seeds[8], 71), 0),
        "up_weight": draw_up_weight(jax.random.fold_in(seeds[8], 71), 0),
        "down_weight": draw_down_weight(jax.random.fold_in(seeds[8], 71), 0),
        "gate_gain": jnp.clip(1.0 + 0.15 * jax.random.normal(seeds[5], (FF,), jnp.float32), 0.25, 1.75),
        "up_gain": jnp.clip(1.0 + 0.15 * jax.random.normal(seeds[6], (FF,), jnp.float32), 0.25, 1.75),
        "down_gain": jnp.clip(1.0 + 0.15 * jax.random.normal(seeds[7], (D,), jnp.float32), 0.25, 1.75),
    }


epsilon = 0.0001
branch_scale = 0.5

def standard(weight, gain):
    raw = weight.astype(jnp.float32)
    cent = raw - lax.optimization_barrier(jnp.mean(raw, axis=0))
    scale = lax.rsqrt(lax.optimization_barrier(jnp.sum(cent * cent, axis=0)) + epsilon)
    hat = (gain.astype(jnp.float32) * cent * scale).astype(jnp.bfloat16)
    return (hat, cent, scale)

def weight_back(grad_hat, gain, cent, scale):
    count = grad_hat.shape[0]
    factor = gain.astype(jnp.float32)
    summed = lax.optimization_barrier(jnp.sum(grad_hat, axis=0))
    crossed = lax.optimization_barrier(jnp.sum(grad_hat * cent, axis=0))
    grad = scale * (factor * grad_hat - factor * summed / count) - scale * scale * scale * cent * (factor * crossed)
    return (grad, scale * crossed)

def rounded(value):
    return lax.optimization_barrier(value.astype(jnp.bfloat16)).astype(jnp.float32)

def reference(tokens, cotangent, gate_weight, up_weight, down_weight, gate_gain, up_gain, down_gain):
    gate_hat, gate_cent, gate_scale = standard(gate_weight, gate_gain)
    up_hat, up_cent, up_scale = standard(up_weight, up_gain)
    down_hat, down_cent, down_scale = standard(down_weight, down_gain)
    scaled = (branch_scale * cotangent.astype(jnp.float32)).astype(jnp.bfloat16)
    width_block = D // N_REPLICA
    gate = jnp.zeros((TOKENS, FF), jnp.float32)
    up = jnp.zeros((TOKENS, FF), jnp.float32)
    dhidden = jnp.zeros((TOKENS, FF), jnp.float32)
    for block_index in range(N_REPLICA):
        start_col = block_index * width_block
        end_col = start_col + width_block
        inputs = tokens[:, start_col:end_col]
        outward = scaled[:, start_col:end_col]
        gate = gate + rounded(jnp.dot(inputs, gate_hat[start_col:end_col], preferred_element_type=jnp.float32))
        up = up + rounded(jnp.dot(inputs, up_hat[start_col:end_col], preferred_element_type=jnp.float32))
        dhidden = dhidden + rounded(jnp.dot(outward, down_hat[:, start_col:end_col].T, preferred_element_type=jnp.float32))
    act = jax.nn.silu(gate)
    hidden = (act * up).astype(jnp.bfloat16)
    sig = jax.nn.sigmoid(gate)
    d_gate = (dhidden * up * sig * (1.0 + gate * (1.0 - sig))).astype(jnp.bfloat16)
    d_up = (dhidden * act).astype(jnp.bfloat16)
    back = jnp.dot(d_gate, gate_hat.T, preferred_element_type=jnp.float32) + jnp.dot(d_up, up_hat.T, preferred_element_type=jnp.float32)
    grad_tokens = cotangent.astype(jnp.float32) + back
    p_gate = jnp.dot(tokens.T, d_gate, preferred_element_type=jnp.float32)
    p_up = jnp.dot(tokens.T, d_up, preferred_element_type=jnp.float32)
    p_down = jnp.dot(hidden.T, scaled, preferred_element_type=jnp.float32)
    grad_gate, grad_gate_gain = weight_back(p_gate, gate_gain, gate_cent, gate_scale)
    grad_up, grad_up_gain = weight_back(p_up, up_gain, up_cent, up_scale)
    grad_down, grad_down_gain = weight_back(p_down, down_gain, down_cent, down_scale)
    return (grad_tokens, grad_gate, grad_up, grad_down, grad_gate_gain, grad_up_gain, grad_down_gain)
```

```python
import functools

import jax
import jax.numpy as jnp
from jax import lax
from jax.experimental import pallas as pl
from jax.sharding import Mesh, PartitionSpec as P

epsilon = 0.0001
branch_scale = 0.5
bf16 = jnp.bfloat16
f32 = jnp.float32


def nn(a, b):
    return lax.dot_general(a, b, (((1,), (0,)), ((), ())), preferred_element_type=f32)


def nt(a, b):
    return lax.dot_general(a, b, (((1,), (1,)), ((), ())), preferred_element_type=f32)


def tn(a, b):
    return lax.dot_general(a, b, (((0,), (0,)), ((), ())), preferred_element_type=f32)


def moments(w):
    mean = jnp.sum(w, axis=0, keepdims=True) * (1.0 / w.shape[0])
    off = w - mean
    return mean, jnp.sum(off * off, axis=0, keepdims=True)


def prepare(gate_ref, up_ref, down_ref, packed_ref, wide_ref, narrow_ref):
    share = packed_ref.shape[2]
    for at, ref in enumerate((gate_ref, up_ref)):
        w = ref[...].astype(f32)
        mean, square = moments(w)
        wide_ref[2 * at : 2 * at + 1, :] = mean
        wide_ref[2 * at + 1 : 2 * at + 2, :] = square
        turned = w.T.astype(bf16)
        for j in range(packed_ref.shape[0]):
            packed_ref[j, at] = turned[j * share : (j + 1) * share]
    w = down_ref[...]
    mean, square = moments(w.astype(f32))
    narrow_ref[0:1, :] = mean
    narrow_ref[1:2, :] = square
    for j in range(packed_ref.shape[0]):
        packed_ref[j, 2] = w[j * share : (j + 1) * share]


def whole(own_ref, other_ref, j, at):
    width = own_ref.shape[-1] // 2
    halves = [
        ref[:, j, :, at * width : (at + 1) * width].reshape(-1, width)
        for ref in (own_ref, other_ref)
    ]
    return jnp.concatenate(halves, axis=0)


def hat_of(w_ref, cols_ref, rows_ref, j, at):
    w = w_ref[j, at].astype(f32)
    if at < 2:
        return ((w - cols_ref[:, 2 * at : 2 * at + 1]) * cols_ref[:, 2 * at + 1 : 2 * at + 2]).astype(bf16)
    return ((w - rows_ref[j, 0:1, :]) * rows_ref[j, 1:2, :]).astype(bf16)


def forward(w_ref, own_ref, other_ref, cols_ref, rows_ref, out_ref):
    blocks = w_ref.shape[0]
    parts = out_ref.shape[0]
    tall = w_ref.shape[2] // parts
    for at in range(3):
        total = None
        for j in range(blocks):
            hat = hat_of(w_ref, cols_ref, rows_ref, j, at)
            term = nt(hat, whole(own_ref, other_ref, j, 0 if at < 2 else 1))
            total = term if total is None else total + term
        total = total.astype(bf16)
        for q in range(parts):
            out_ref[q, at * tall : (at + 1) * tall, :] = total[q * tall : (q + 1) * tall]
    ones = jnp.ones((8, own_ref.shape[-1] // 2), bf16)
    row = None
    for j in range(blocks):
        term = nt(ones, whole(own_ref, other_ref, j, 0))
        row = term if row is None else row + term
    high = row.astype(bf16)
    low = (row - high.astype(f32)).astype(bf16)
    index = lax.broadcasted_iota(jnp.int32, row.shape, 0)
    both = jnp.where(index == 0, high.astype(f32), jnp.where(index == 1, low.astype(f32), 0.0)).astype(bf16)
    for q in range(parts):
        out_ref[q, 3 * tall : 3 * tall + 8, :] = both


def gating(z_ref, d_ref, dots_ref, row_ref):
    tall = dots_ref.shape[0]

    def summed(a, b):
        total = z_ref[0, a:b, :].astype(f32)
        for q in range(1, z_ref.shape[0]):
            total = total + z_ref[q, a:b, :].astype(f32)
        return total

    gate = summed(0, tall)
    up = summed(tall, 2 * tall)
    dhidden = summed(2 * tall, 3 * tall)
    row = summed(3 * tall, 3 * tall + 8)
    row_ref[...] = jnp.broadcast_to(row[0:1] + row[1:2], row_ref.shape)
    sig = 1.0 / (1.0 + jnp.exp(-gate))
    act = gate * sig
    d_gate = (dhidden * up * sig * (1.0 + gate * (1.0 - sig))).astype(bf16)
    d_up = (dhidden * act).astype(bf16)
    d_ref[0:tall, :] = d_gate
    d_ref[tall : 2 * tall, :] = d_up
    d_ref[2 * tall : 3 * tall, :] = (act * up).astype(bf16)
    gate_dot = jnp.sum(d_gate.astype(f32) * gate, axis=1, keepdims=True)
    up_dot = jnp.sum(d_up.astype(f32) * up, axis=1, keepdims=True)
    lane = lax.broadcasted_iota(jnp.int32, dots_ref.shape, 1)
    dots_ref[...] = jnp.where(lane == 0, gate_dot, jnp.where(lane == 1, up_dot, 0.0))


def backward(
    width_all, d_ref, w_ref, own_ref, other_ref, cols_ref, rows_ref, dots_ref, row_ref,
    grad_ref, sums_ref, mine_ref, theirs_ref,
):
    blocks = w_ref.shape[0]
    parts = d_ref.shape[0]
    tall = w_ref.shape[2] // parts
    streams = [
        jnp.concatenate([d_ref[q, at * tall : (at + 1) * tall, :] for q in range(parts)], axis=0)
        for at in range(3)
    ]
    row = row_ref[0:1, :]
    means = [
        jnp.sum(streams[at].astype(f32) * row, axis=1, keepdims=True) * (1.0 / width_all) for at in range(2)
    ]
    half = mine_ref.shape[0] * mine_ref.shape[2]
    for j in range(blocks):
        left = whole(own_ref, other_ref, j, 0)
        back = None
        for at in range(2):
            p = nn(streams[at], left)
            gs = cols_ref[:, 2 * at + 1 : 2 * at + 2]
            s = cols_ref[:, 4 + at : 5 + at]
            cent = w_ref[j, at].astype(f32) - cols_ref[:, 2 * at : 2 * at + 1]
            grad = gs * (p - means[at]) - cent * (s * s * dots_ref[:, at : at + 1])
            grad_ref[j, at] = grad.astype(bf16)
            term = tn(streams[at], (cent * gs).astype(bf16))
            back = term if back is None else back + term
        mine_ref[:, j] = back[:half].reshape(mine_ref.shape[0], mine_ref.shape[2], mine_ref.shape[3])
        theirs_ref[:, j] = (
            back[half:].astype(bf16).reshape(mine_ref.shape[0], mine_ref.shape[2], mine_ref.shape[3])
        )
        p = nn(streams[2], whole(own_ref, other_ref, j, 1))
        cent = w_ref[j, 2].astype(f32) - rows_ref[j, 0:1, :]
        sums_ref[j, 0:1, :] = jnp.sum(p, axis=0, keepdims=True)
        sums_ref[j, 1:2, :] = jnp.sum(p * cent, axis=0, keepdims=True)
        grad_ref[j, 2] = p.astype(bf16)


def finish(hidden_all, g_ref, down_ref, stat_ref, gate_ref, up_ref, grad_ref):
    for at, ref in enumerate((gate_ref, up_ref)):
        tall = jnp.concatenate([g_ref[j, at].astype(f32) for j in range(g_ref.shape[0])], axis=0)
        ref[...] = tall.T
    mean, s, gain = stat_ref[0:1, :], stat_ref[1:2, :], stat_ref[2:3, :]
    summed, crossed = stat_ref[3:4, :], stat_ref[4:5, :]
    share = g_ref.shape[2]
    for j in range(g_ref.shape[0]):
        p = g_ref[j, 2].astype(f32)
        cent = down_ref[j * share : (j + 1) * share, :].astype(f32) - mean
        grad_ref[j * share : (j + 1) * share, :] = s * gain * (p - summed * (1.0 / hidden_all)) - (
            s * s * s * gain * crossed
        ) * cent


def call(body, outs, *args):
    return pl.pallas_call(body, out_shape=[jax.ShapeDtypeStruct(s, t) for s, t in outs])(*args)


def exchange(x, axis):
    return lax.all_to_all(x, axis, split_axis=0, concat_axis=0, tiled=True)


def to_all(x, axis):
    size = 1
    for a in (axis,) if isinstance(axis, str) else axis:
        size *= lax.axis_size(a)
    return exchange(jnp.broadcast_to(x, (size, *x.shape)), axis)


def combined(means, squares, count):
    mean = jnp.mean(means, axis=0)
    off = means - mean
    return mean, lax.rsqrt(jnp.sum(squares, axis=0) + count * jnp.sum(off * off, axis=0) + epsilon)


BLK = ("y", "zl", "core")
REP = ("zh", "x")


def local(tokens, cotangent, gate_weight, up_weight, down_weight, gate_gain, up_gain, down_gain):
    rows, width = tokens.shape
    hidden = gate_weight.shape[1]
    nx, nz, ny = lax.axis_size("x"), lax.axis_size("zh"), lax.axis_size("y")
    nl = lax.axis_size("zl")
    width_all = width * nx * nz
    hidden_all = hidden * ny * nl * lax.axis_size("core")
    share = hidden // nx
    tall = share // nz
    count = rows * ny * nl * lax.axis_size("core")
    me = lax.axis_index("x")

    scaled = (branch_scale * cotangent.astype(f32)).astype(bf16)
    both = jnp.concatenate([tokens, scaled], axis=1)
    along = to_all(both, "x")
    packed, wide, narrow = call(
        prepare,
        [((nx, 3, share, width), bf16), ((4, hidden), f32), ((2, width), f32)],
        gate_weight, up_weight, down_weight,
    )
    along = to_all(along, "zl")
    along = jnp.moveaxis(along, 0, 1).reshape(nx, nl * rows, 2 * width)
    weights = exchange(packed, "x")

    own = to_all(along, "y")
    other = lax.ppermute(own, "core", [(0, 1), (1, 0)])

    wide = jnp.moveaxis(wide.reshape(4, nx, share), 1, 0)
    wide = exchange(jnp.broadcast_to(wide[None], (nz, nx, 4, share)).reshape(nz * nx, 4, share), REP)
    gate_mean, gate_scale = combined(wide[:, 0], wide[:, 1], width)
    up_mean, up_scale = combined(wide[:, 2], wide[:, 3], width)
    my_gate_gain = gate_gain.reshape(nx, share)[me]
    my_up_gain = up_gain.reshape(nx, share)[me]
    cols = jnp.stack(
        [
            gate_mean, my_gate_gain * gate_scale, up_mean, my_up_gain * up_scale,
            gate_scale, up_scale, gate_scale, up_scale,
        ],
        axis=1,
    )
    narrow = to_all(narrow, BLK)
    down_mean, down_scale = combined(narrow[:, 0], narrow[:, 1], hidden)
    rows_of = to_all(jnp.stack([down_mean, down_gain * down_scale]), "x")

    (parts,) = call(
        forward, [((nz, 3 * tall + 8, count), bf16)], weights, own, other, cols, rows_of
    )
    parts = exchange(parts, "zh")
    d, dots, row = call(
        gating, [((3 * tall, count), bf16), ((tall, 128), f32), ((8, count), f32)], parts
    )
    dots = to_all(dots, "zh").reshape(share, 128)
    d = to_all(d, "zh")
    shape = (ny, nx, nl * rows, width)
    grads, sums, mine, theirs = call(
        functools.partial(backward, width_all),
        [((nx, 3, share, width), bf16), ((nx, 2, width), f32), (shape, f32), (shape, bf16)],
        d, weights, own, other, cols, rows_of, dots, row,
    )
    theirs = lax.ppermute(theirs, "core", [(0, 1), (1, 0)])
    sums = exchange(sums, "x").sum(axis=0)
    sums = to_all(sums, BLK).sum(axis=0)
    gains = to_all(dots[:, :2].T, "x")
    gains = jnp.moveaxis(gains, 0, 1).reshape(2, hidden)
    grads = exchange(grads, "x")
    back = exchange((mine + theirs.astype(f32)).astype(bf16), "y")
    back = back.astype(f32).sum(axis=0).astype(bf16)
    back = jnp.moveaxis(back.reshape(nx, nl, rows, width), 1, 0)
    back = exchange(back, "zl").astype(f32).sum(axis=0).astype(bf16)
    back = exchange(back, "x").astype(f32).sum(axis=0)
    grad_tokens = cotangent.astype(f32) + back
    zero = jnp.zeros_like(down_mean)
    stat = jnp.stack([down_mean, down_scale, down_gain, sums[0], sums[1], zero, zero, zero])
    grad_gate, grad_up, grad_down = call(
        functools.partial(finish, hidden_all),
        [((width, hidden), f32), ((width, hidden), f32), ((hidden, width), f32)],
        grads, down_weight, stat,
    )
    return (
        grad_tokens,
        grad_gate,
        grad_up,
        grad_down,
        gains[0] / gate_gain,
        gains[1] / up_gain,
        down_scale * sums[1],
    )


def solution(mesh):
    fine = Mesh(mesh.devices.reshape(4, 4, 2, 4, 4), (*BLK, *REP))
    return jax.shard_map(
        local,
        mesh=fine,
        in_specs=(
            P(BLK, REP), P(BLK, REP), P(REP, BLK), P(REP, BLK), P(BLK, REP), P(BLK), P(BLK), P(REP),
        ),
        out_specs=(
            P(BLK, REP), P(REP, BLK), P(REP, BLK), P(BLK, REP), P(BLK), P(BLK), P(REP),
        ),
        check_vma=False,
    )
```

```python
import functools

import jax
import jax.numpy as jnp
from jax import lax
from jax.experimental import pallas as pl
from jax.experimental.pallas import tpu as pltpu
from jax.sharding import Mesh, PartitionSpec as P


epsilon = 0.0001
branch_scale = 0.5
bf16 = jnp.bfloat16
f32 = jnp.float32

BLK = ("y", "zl", "core")
REP = ("zh", "x")


def nn(a, b):
    return lax.dot_general(a, b, (((1,), (0,)), ((), ())), preferred_element_type=f32)


def nt(a, b):
    return lax.dot_general(a, b, (((1,), (1,)), ((), ())), preferred_element_type=f32)


def tn(a, b):
    return lax.dot_general(a, b, (((0,), (0,)), ((), ())), preferred_element_type=f32)


def pieces(x):
    high = x.astype(bf16)
    rest = x - high.astype(f32)
    middle = rest.astype(bf16)
    return high, middle, (rest - middle.astype(f32)).astype(bf16)


def joined(rows):
    return rows[0:1].astype(f32) + rows[1:2].astype(f32) + rows[2:3].astype(f32)


def merged(moments, count):
    mean = sum(m for m, _ in moments) * (1.0 / len(moments))
    square = sum(s for _, s in moments)
    for m, _ in moments:
        square = square + count * ((m - mean) * (m - mean))
    return mean, square


def upright(row, tall):
    shape = (tall, row.shape[1])
    same = lax.broadcasted_iota(jnp.int32, shape, 0) == lax.broadcasted_iota(jnp.int32, shape, 1)
    return jnp.sum(jnp.where(same, row, 0.0), axis=1, keepdims=True)


def level(col, wide):
    shape = (col.shape[0], wide)
    same = lax.broadcasted_iota(jnp.int32, shape, 0) == lax.broadcasted_iota(jnp.int32, shape, 1)
    return jnp.sum(jnp.where(same, col, 0.0), axis=0, keepdims=True)


def pack_tokens(tokens_ref, cotangent_ref, gate_ref, up_ref, down_ref, gain_ref, out_ref):
    rows, width = tokens_ref.shape
    scaled = (branch_scale * cotangent_ref[...].astype(f32)).astype(bf16)

    def moments(ref):
        w = ref[...].astype(f32)
        mean = jnp.sum(w, axis=0, keepdims=True) * (1.0 / w.shape[0])
        off = w - mean
        return mean, jnp.sum(off * off, axis=0, keepdims=True)

    def single(x):
        return [p.astype(f32) for p in pieces(x)]

    mean, square = moments(down_ref)
    gain = single(gain_ref[...])
    left = jnp.concatenate([tokens_ref[...].astype(f32), *single(mean), gain[0]], axis=0).astype(bf16)
    right = jnp.concatenate([scaled.astype(f32), *single(square), gain[1]], axis=0).astype(bf16)
    wide = [moments(ref) for ref in (gate_ref, up_ref)]
    blocks, lines = out_ref.shape[0], out_ref.shape[1]
    share = gate_ref.shape[1] // blocks
    for j in range(blocks):
        sides = []
        for side in range(2):
            parts = []
            for pair in wide:
                row = pair[side][:, j * share : (j + 1) * share]
                parts += single(jnp.concatenate([row, jnp.zeros((1, width - share), f32)], axis=1))
            sides.append(jnp.concatenate([*parts, jnp.zeros((2, width), f32)], axis=0).astype(bf16))
        for l in range(lines):
            out_ref[j, l, 0 : rows + 4, 0:width] = left
            out_ref[j, l, 0 : rows + 4, width : 2 * width] = right
            out_ref[j, l, rows + 4 : rows + 12, 0:width] = sides[0]
            out_ref[j, l, rows + 4 : rows + 12, width : 2 * width] = sides[1]


def pack_weights(place_ref, gate_ref, up_ref, down_ref, *refs):
    *outs, store_ref = refs
    blocks, _, share, _ = store_ref.shape
    for at, ref in enumerate((gate_ref, up_ref)):
        turned = ref[...].astype(f32).T.astype(bf16)
        for j in range(blocks):
            store_ref[j, at] = turned[j * share : (j + 1) * share]
    for j in range(blocks):
        store_ref[j, 2] = down_ref[j * share : (j + 1) * share]
    for k in range(blocks):
        outs[k][...] = store_ref[lax.rem(place_ref[1] + k, blocks)]


def repack_tokens(wide_count, tall_count, place_ref, in_ref, out_ref, moment_ref):
    blocks, lines, high, wide = in_ref.shape
    rows = high - 12
    width = wide // 2
    for j in range(blocks):
        source = lax.rem(place_ref[1] + blocks - j, blocks)
        lots = [in_ref[source, l, 0 : rows + 4, :].astype(f32) for l in range(lines)]
        moments = [
            (joined(lot[rows : rows + 3, 0:width]), joined(lot[rows : rows + 3, width:])) for lot in lots
        ]
        mean, square = merged(moments, tall_count)
        zero = jnp.zeros((4, width), f32)
        for extra, a in ((mean, 0), (square, width)):
            parts = [lot[0:rows, a : a + width] for lot in lots]
            parts += [p.astype(f32) for p in pieces(extra)]
            parts += [lots[0][rows + 3 : rows + 4, a : a + width], zero]
            block = jnp.concatenate(parts, axis=0).astype(bf16)
            for y in range(out_ref.shape[0]):
                out_ref[y, j, :, a : a + width] = block
    line = place_ref[2]
    own = [in_ref[j, line, rows + 4 : rows + 12, :].astype(f32) for j in range(blocks)]
    found = []
    for at in range(2):
        moments = [
            (joined(o[3 * at : 3 * at + 3, 0:width]), joined(o[3 * at : 3 * at + 3, width:])) for o in own
        ]
        found += merged(moments, wide_count)
    block = jnp.concatenate([*found, jnp.zeros((4, width), f32)], axis=0)
    moment_ref[...] = block


def whole(own_ref, other_ref, j, at):
    rows = own_ref.shape[2] - 8
    width = own_ref.shape[3] // 2
    halves = [
        ref[:, j, 0:rows, at * width : (at + 1) * width].reshape(-1, width) for ref in (own_ref, other_ref)
    ]
    return jnp.concatenate(halves, axis=0)


def forward(
    wide_count, tall_count, place_ref, w0_ref, w1_ref, w2_ref, w3_ref, own_ref, other_ref,
    moment0_ref, moment1_ref, moment2_ref, moment3_ref, gain_ref,
    kept_ref, near_a_ref, near_b_ref, back_a_ref, back_b_ref, far_a_ref, far_b_ref,
    cols_ref, rows_ref, row_ref, store_ref,
):
    w_ref = (w0_ref, w1_ref, w2_ref, w3_ref)
    blocks = len(w_ref)
    _, share, width = w0_ref.shape
    parts = store_ref.shape[0]
    tall = share // parts
    lane = lax.broadcasted_iota(jnp.int32, cols_ref.shape, 1)
    cols = jnp.zeros(cols_ref.shape, f32)
    row = 0.0
    lefts = [whole(own_ref, other_ref, j, 0) for j in range(blocks)]
    ones = jnp.ones((8, width), bf16)
    for j in range(blocks):
        row = row + nt(ones, lefts[j])
    row_ref[...] = row
    for at in range(2):
        moments = [
            (ref[2 * at : 2 * at + 1, :], ref[2 * at + 1 : 2 * at + 2, :])
            for ref in (moment0_ref, moment1_ref, moment2_ref, moment3_ref)
        ]
        mean, square = merged(moments, wide_count)
        mean = upright(mean, share)
        scale = upright(lax.rsqrt(square + epsilon), share)
        gs = gain_ref[:, at : at + 1] * scale
        for k, v in ((3 * at, mean), (3 * at + 1, gs), (3 * at + 2, scale)):
            cols = jnp.where(lane == k, v, cols)
        total = 0.0
        for j in range(blocks):
            total = total + nt(w_ref[j][at], lefts[j])
        total = ((total - mean * row[0:1]) * gs).astype(bf16)
        for q in range(parts):
            store_ref[q, at * tall : (at + 1) * tall, :] = total[q * tall : (q + 1) * tall]
    cols_ref[...] = cols
    total = 0.0
    rows = own_ref.shape[2] - 8
    for j in range(blocks):
        lots = [
            ref[y, j, rows : rows + 8, :].astype(f32) for ref in (own_ref, other_ref) for y in range(own_ref.shape[0])
        ]
        mean, square = merged([(joined(lot[:, 0:width]), joined(lot[:, width:])) for lot in lots], tall_count)
        scale = lax.rsqrt(square + epsilon)
        gain = lots[0][3:4, 0:width] + lots[0][3:4, width:]
        gs = gain * scale
        rows_ref[j] = jnp.concatenate([mean, gs, scale, jnp.zeros((5, width), f32)], axis=0)
        hat = ((w_ref[j][2].astype(f32) - mean) * gs).astype(bf16)
        total = total + nt(hat, whole(own_ref, other_ref, j, 1))
    total = total.astype(bf16)
    for q in range(parts):
        store_ref[q, 2 * tall : 3 * tall, :] = total[q * tall : (q + 1) * tall]
    at = place_ref[0]
    cut = near_a_ref.shape[0]
    kept_ref[...] = store_ref[at]
    for k, a_ref, b_ref in ((1, near_a_ref, near_b_ref), (2, far_a_ref, far_b_ref), (3, back_a_ref, back_b_ref)):
        q = lax.rem(at + k, parts)
        a_ref[...] = store_ref[q, 0:cut, :]
        b_ref[...] = store_ref[q, cut:, :]


def add_pair(a_ref, b_ref, c_ref, d_ref, left_ref, right_ref):
    left_ref[...] = (a_ref[...].astype(f32) + b_ref[...].astype(f32)).astype(bf16)
    right_ref[...] = (c_ref[...].astype(f32) + d_ref[...].astype(f32)).astype(bf16)


def gating(kept_ref, near_a_ref, near_b_ref, back_a_ref, back_b_ref, row_ref, d_ref):
    tall = (d_ref.shape[0] - 8) // 3
    cut = near_a_ref.shape[0]
    top = kept_ref[0:cut, :].astype(f32) + near_a_ref[...].astype(f32) + back_a_ref[...].astype(f32)
    low = kept_ref[cut:, :].astype(f32) + near_b_ref[...].astype(f32) + back_b_ref[...].astype(f32)
    total = jnp.concatenate([top, low], axis=0)
    gate, up, dhidden = total[0:tall], total[tall : 2 * tall], total[2 * tall : 3 * tall]
    sig = 1.0 / (1.0 + jnp.exp(-gate))
    act = gate * sig
    d_gate = (dhidden * up * sig * (1.0 + gate * (1.0 - sig))).astype(bf16)
    d_up = (dhidden * act).astype(bf16)
    d_ref[2 * tall : 3 * tall, :] = (act * up).astype(bf16)
    d_ref[0:tall, :] = d_gate
    d_ref[tall : 2 * tall, :] = d_up
    dots = [
        level(jnp.sum(d.astype(f32) * v, axis=1, keepdims=True), 128)
        for d, v in ((d_gate, gate), (d_up, up))
    ]
    wide = d_ref.shape[1]
    dots = jnp.concatenate([*dots, jnp.zeros((1, wide - 256), f32)], axis=1)
    extra = [*pieces(dots), *pieces(row_ref[0:1, :])]
    extra = [p.astype(f32) for p in extra] + [jnp.zeros((2, wide), f32)]
    d_ref[3 * tall : 3 * tall + 8, :] = jnp.concatenate(extra, axis=0).astype(bf16)


def stacked(d_ref, at, tall):
    return jnp.concatenate(
        [d_ref[q, at * tall : (at + 1) * tall, :] for q in range(d_ref.shape[0])], axis=0
    )


def token_back(d_ref, w0_ref, w1_ref, w2_ref, w3_ref, cols_ref, mine_ref, theirs_ref):
    w_ref = (w0_ref, w1_ref, w2_ref, w3_ref)
    blocks = len(w_ref)
    _, share, width = w0_ref.shape
    tall = share // d_ref.shape[0]
    streams = [stacked(d_ref, at, tall) for at in range(2)]
    lines, _, rows, _ = mine_ref.shape
    half = lines * rows
    for j in range(blocks):
        back = 0.0
        for at in range(2):
            cent = w_ref[j][at].astype(f32) - cols_ref[:, 3 * at : 3 * at + 1]
            back = back + tn(streams[at], (cent * cols_ref[:, 3 * at + 1 : 3 * at + 2]).astype(bf16))
        mine_ref[:, j] = back[:half].reshape(lines, rows, width)
        theirs_ref[:, j] = back[half:].astype(bf16).reshape(lines, rows, width)


def tall_grads(d_ref, w0_ref, w1_ref, w2_ref, w3_ref, own_ref, other_ref, rows_ref, grad_ref, sums_ref):
    w_ref = (w0_ref, w1_ref, w2_ref, w3_ref)
    blocks = len(w_ref)
    _, share, width = w0_ref.shape
    stream = stacked(d_ref, 2, share // d_ref.shape[0])
    for j in range(blocks):
        p = nn(stream, whole(own_ref, other_ref, j, 1))
        cent = w_ref[j][2].astype(f32) - rows_ref[j, 0:1, :]
        summed = jnp.sum(p, axis=0, keepdims=True)
        crossed = jnp.sum(p * cent, axis=0, keepdims=True)
        sums_ref[j] = jnp.concatenate([summed, crossed, jnp.zeros((6, width), f32)], axis=0)
        grad_ref[j] = p.astype(bf16)


def wide_grads(width_all, d_ref, w0_ref, w1_ref, w2_ref, w3_ref, own_ref, other_ref, cols_ref, down_ref, g0_ref, g1_ref, g2_ref, g3_ref, dots_ref):
    w_ref = (w0_ref, w1_ref, w2_ref, w3_ref)
    grad_ref = (g0_ref, g1_ref, g2_ref, g3_ref)
    blocks = len(w_ref)
    _, share, _ = w0_ref.shape
    parts = d_ref.shape[0]
    tall = share // parts
    streams = [stacked(d_ref, at, tall) for at in range(2)]
    extra = [d_ref[q, 3 * tall : 3 * tall + 8, :].astype(f32) for q in range(parts)]
    row = sum(joined(e[3:6]) for e in extra)
    dots_ref[...] = jnp.zeros(dots_ref.shape, f32)
    means, pulls = [], []
    for at in range(2):
        means.append(jnp.sum(streams[at].astype(f32) * row, axis=1, keepdims=True) * (1.0 / width_all))
        dot = jnp.concatenate(
            [upright(joined(e[0:3, 128 * at : 128 * (at + 1)]), tall) for e in extra], axis=0
        )
        dots_ref[at : at + 1, :] = level(dot, dots_ref.shape[1])
        s = cols_ref[:, 3 * at + 2 : 3 * at + 3]
        pulls.append(s * s * dot)
    for j in range(blocks):
        left = whole(own_ref, other_ref, j, 0)
        for at in range(2):
            p = nn(streams[at], left)
            cent = w_ref[j][at].astype(f32) - cols_ref[:, 3 * at : 3 * at + 1]
            grad = cols_ref[:, 3 * at + 1 : 3 * at + 2] * (p - means[at]) - cent * pulls[at]
            grad_ref[j][at] = grad.astype(bf16)
        grad_ref[j][2] = down_ref[j]


def both_cores(mine_ref, theirs_ref, sums_ref, other_ref, out_ref):
    lines, blocks, rows, _ = mine_ref.shape
    for j in range(blocks):
        total = sums_ref[j] + other_ref[j]
        extra = [p.astype(f32) for k in range(2) for p in pieces(total[k : k + 1, :])]
        extra = jnp.concatenate([*extra, total[2:4, :]], axis=0).astype(bf16)
        for y in range(lines):
            out_ref[y, j, 0:rows, :] = (mine_ref[y, j] + theirs_ref[y, j].astype(f32)).astype(bf16)
            out_ref[y, j, rows : rows + 8, :] = extra


def whole_column(place_ref, in_ref, dots_ref, out_ref):
    lines, blocks, high, _ = in_ref.shape
    dots = [p.astype(f32) for k in range(2) for p in pieces(dots_ref[k : k + 1, :])]
    cuts = out_ref.shape[0]
    rows = (high - 8) // cuts
    for j in range(blocks):
        lots = [in_ref[y, j].astype(f32) for y in range(lines)]
        back = sum(lot[0 : high - 8] for lot in lots)
        extra = []
        for k in range(2):
            total = sum(joined(lot[high - 8 + 3 * k : high - 5 + 3 * k]) for lot in lots)
            extra += [p.astype(f32) for p in pieces(total)]
        for l in range(cuts):
            out_ref[l, lax.rem(place_ref[1] + blocks - j, blocks)] = jnp.concatenate([back[l * rows : (l + 1) * rows], *extra, *dots], axis=0).astype(bf16)


def finish_wide(place_ref, g0_ref, g1_ref, g2_ref, g3_ref, gate_ref, up_ref, store_ref):
    g_ref = (g0_ref, g1_ref, g2_ref, g3_ref)
    for at, ref in enumerate((gate_ref, up_ref)):
        for k, g in enumerate(g_ref):
            store_ref[lax.rem(place_ref[1] + k, len(g_ref))] = g[at].astype(f32)
        ref[...] = store_ref[...].reshape(-1, store_ref.shape[2]).T


def finish_tall(
    hidden_all, place_ref, in_ref, cotangent_ref, g0_ref, g1_ref, g2_ref, g3_ref, down_ref, rows_ref, gain_ref,
    tokens_ref, grad_ref, dgain_ref, dots_ref,
):
    lines, blocks, _, _ = in_ref.shape
    rows = tokens_ref.shape[0]
    lots = [in_ref[l, j].astype(f32) for l in range(lines) for j in range(blocks)]
    total = sum(lots)
    tokens_ref[...] = cotangent_ref[...].astype(f32) + total[0:rows]
    summed, crossed = (sum(joined(lot[rows + 3 * k : rows + 3 * k + 3]) for lot in lots) for k in range(2))
    line = place_ref[2]
    for j in range(blocks):
        own = in_ref[line, j].astype(f32)
        dots_ref[0:1, j, :] = joined(own[rows + 6 : rows + 9])
        dots_ref[1:2, j, :] = joined(own[rows + 9 : rows + 12])
    mine = rows_ref[0]
    mean, scale = mine[0:1, :], mine[2:3, :]
    gain = gain_ref[...]
    dgain_ref[...] = scale * crossed
    g_ref = (g0_ref, g1_ref, g2_ref, g3_ref)
    for k, g in enumerate(g_ref):
        j = lax.rem(place_ref[1] + k, len(g_ref))
        cent = down_ref[j].astype(f32) - mean
        grad_ref[j] = scale * gain * (g[2].astype(f32) - summed * (1.0 / hidden_all)) - (
            scale * scale * scale * gain * crossed
        ) * cent


def call(body, outs, *args, place=None, scratch=()):
    specs = [pl.BlockSpec(memory_space=pltpu.VMEM)] * len(args)
    if place is not None:
        args = (place, *args)
        specs = [pl.BlockSpec(memory_space=pltpu.SMEM), *specs]
    return pl.pallas_call(
        body,
        out_shape=[jax.ShapeDtypeStruct(s, t) for s, t in outs],
        in_specs=specs,
        scratch_shapes=scratch,
    )(*args)


def exchange(x, axis):
    return lax.all_to_all(x, axis, split_axis=0, concat_axis=0, tiled=True)


def shift(x, axis, by):
    size = lax.axis_size(axis)
    return lax.ppermute(x, axis, [(i, (i + by) % size) for i in range(size)])


def block(tokens, cotangent, gate_weight, up_weight, down_weight, gate_gain, up_gain, down_gain):
    rows, width = tokens.shape
    hidden = gate_weight.shape[1]
    nx, nz, ny = lax.axis_size("x"), lax.axis_size("zh"), lax.axis_size("y")
    nl, nc = lax.axis_size("zl"), lax.axis_size("core")
    width_all = width * nx * nz
    hidden_all = hidden * ny * nl * nc
    share = hidden // nx
    tall = share // nz
    count = rows * ny * nl * nc
    place = jnp.stack([lax.axis_index("zh"), lax.axis_index("x"), lax.axis_index("zl")]).astype(jnp.int32)
    swap = [(0, 1), (1, 0)]

    def grid_exchange(x, axes):
        flat = exchange(x.reshape(x.shape[0] * x.shape[1], *x.shape[2:]), axes)
        return flat.reshape(x.shape)

    (both,) = call(
        pack_tokens, [((nx, nl, rows + 12, 2 * width), bf16)],
        tokens, cotangent, gate_weight, up_weight, down_weight, down_gain.reshape(1, width),
    )
    both = grid_exchange(both, ("x", "zl"))
    cut_weights = call(
        pack_weights, [((3, share, width), bf16)] * nx, gate_weight, up_weight, down_weight,
        place=place, scratch=[pltpu.VMEM((nx, 3, share, width), bf16)],
    )
    weights = [cut_weights[0], *(shift(cut_weights[k], "x", k) for k in (1, 2, 3))]
    both, moments = call(
        functools.partial(repack_tokens, width, hidden),
        [((ny, nx, nl * rows + 8, 2 * width), bf16), ((8, width), f32)], both, place=place,
    )
    own = exchange(both, "y")
    moments = [moments, *(shift(moments, "zh", k) for k in (1, 2, 3))]
    other = lax.ppermute(own, "core", swap)
    gains = jnp.stack([gate_gain.reshape(nx, share)[place[1]], up_gain.reshape(nx, share)[place[1]]], axis=1)

    cut = 88
    a, b = ((cut, count), bf16), ((3 * tall - cut, count), bf16)
    kept, near_a, near_b, back_a, back_b, far_a, far_b, cols, rows_of, row = call(
        functools.partial(forward, width * nx, hidden * nl),
        [
            ((3 * tall, count), bf16), a, b, a, b, a, b,
            ((share, 128), f32), ((nx, 8, width), f32), ((8, count), f32),
        ],
        *weights, own, other, *moments, gains,
        place=place,
        scratch=[pltpu.VMEM((nz, 3 * tall, count), bf16)],
    )
    far_a = shift(far_a, "zh", 1)
    far_b = shift(far_b, "zh", -1)
    near_b = shift(near_b, "zh", 1)
    back_a = shift(back_a, "zh", -1)
    near_a, back_b = call(add_pair, [a, b], near_a, far_a, back_b, far_b)
    near_a = shift(near_a, "zh", 1)
    back_b = shift(back_b, "zh", -1)
    (d,) = call(gating, [((3 * tall + 8, count), bf16)], kept, near_a, near_b, back_a, back_b, row)
    d = lax.all_gather(d, "zh")

    shape = (ny, nx, nl * rows, width)
    mine, theirs = call(token_back, [(shape, f32), (shape, bf16)], d, *weights, cols)
    theirs = lax.ppermute(theirs, "core", swap)
    down_grads, sums = call(
        tall_grads, [((nx, share, width), bf16), ((nx, 8, width), f32)], d, *weights, own, other, rows_of
    )
    other_sums = lax.ppermute(sums, "core", swap)
    (back,) = call(both_cores, [((ny, nx, nl * rows + 8, width), bf16)], mine, theirs, sums, other_sums)
    back = exchange(back, "y")
    *grads, dots = call(
        functools.partial(wide_grads, width_all), [((3, share, width), bf16)] * nx + [((8, width), f32)],
        d, *weights, own, other, cols, down_grads,
    )
    grads = [grads[0], *(shift(grads[k], "x", -k) for k in (1, 2, 3))]
    (back,) = call(whole_column, [((nl, nx, rows + 12, width), bf16)], back, dots, place=place)
    back = grid_exchange(back, ("zl", "x"))
    grad_gate, grad_up = call(
        finish_wide, [((width, hidden), f32), ((width, hidden), f32)], *grads,
        place=place, scratch=[pltpu.VMEM((nx, share, width), f32)],
    )
    grad_tokens, grad_down, down_dgain, dots = call(
        functools.partial(finish_tall, hidden_all),
        [((rows, width), f32), ((nx, share, width), f32), ((1, width), f32), ((2, nx, width), f32)],
        back, cotangent, *grads, down_weight.reshape(nx, share, width), rows_of, down_gain.reshape(1, width),
        place=place,
    )
    dots = dots[:, :, :share].reshape(2, hidden)
    return (
        grad_tokens,
        grad_gate,
        grad_up,
        grad_down.reshape(hidden, width),
        dots[0] / gate_gain,
        dots[1] / up_gain,
        down_dgain.reshape(width),
    )


def solution(mesh):
    fine = Mesh(mesh.devices.reshape(4, 4, 2, 4, 4), (*BLK, *REP))
    return jax.shard_map(
        block,
        mesh=fine,
        in_specs=(
            P(BLK, REP), P(BLK, REP), P(REP, BLK), P(REP, BLK), P(BLK, REP), P(BLK), P(BLK), P(REP),
        ),
        out_specs=(
            P(BLK, REP), P(REP, BLK), P(REP, BLK), P(BLK, REP), P(BLK), P(BLK), P(REP),
        ),
        check_vma=False,
    )
```

```python
import functools

import jax
import jax.numpy as jnp
from jax import lax
from jax.experimental import pallas as pl
from jax.experimental.pallas import tpu as pltpu
from jax.sharding import Mesh, PartitionSpec as P


epsilon = 0.0001
branch_scale = 0.5
bf16 = jnp.bfloat16
f32 = jnp.float32

BLK = ("y", "zl", "core")
REP = ("zh", "x")


def nn(a, b):
    return lax.dot_general(a, b, (((1,), (0,)), ((), ())), preferred_element_type=f32)


def nt(a, b):
    return lax.dot_general(a, b, (((1,), (1,)), ((), ())), preferred_element_type=f32)


def pieces(x):
    high = x.astype(bf16)
    rest = x - high.astype(f32)
    middle = rest.astype(bf16)
    return high, middle, (rest - middle.astype(f32)).astype(bf16)


def joined(rows):
    return rows[0:1].astype(f32) + rows[1:2].astype(f32) + rows[2:3].astype(f32)


def merged(moments, count):
    mean = sum(m for m, _ in moments) * (1.0 / len(moments))
    square = sum(s for _, s in moments)
    for m, _ in moments:
        square = square + count * ((m - mean) * (m - mean))
    return mean, square


def upright(row, tall):
    shape = (tall, row.shape[1])
    same = lax.broadcasted_iota(jnp.int32, shape, 0) == lax.broadcasted_iota(jnp.int32, shape, 1)
    return jnp.sum(jnp.where(same, row, 0.0), axis=1, keepdims=True)


def level(col, wide):
    shape = (col.shape[0], wide)
    same = lax.broadcasted_iota(jnp.int32, shape, 0) == lax.broadcasted_iota(jnp.int32, shape, 1)
    return jnp.sum(jnp.where(same, col, 0.0), axis=0, keepdims=True)


def fetched(pairs, sems):
    copies = [pltpu.make_async_copy(a, b, sems.at[i]) for i, (a, b) in enumerate(pairs)]
    for c in copies:
        c.start()
    return copies


def pack_tokens(
    down_hbm, gain_hbm, tokens_hbm, cotangent_hbm, gate_hbm, up_hbm, out_ref,
    down_ref, gain_ref, tokens_ref, cotangent_ref, gate_ref, up_ref, sems,
):
    copies = fetched(
        (
            (down_hbm, down_ref), (gain_hbm, gain_ref), (tokens_hbm, tokens_ref), (cotangent_hbm, cotangent_ref),
            (gate_hbm, gate_ref), (up_hbm, up_ref),
        ),
        sems,
    )
    rows, width = tokens_ref.shape

    def moments(ref):
        w = ref[...].astype(f32)
        mean = jnp.sum(w, axis=0, keepdims=True) * (1.0 / w.shape[0])
        off = w - mean
        return mean, jnp.sum(off * off, axis=0, keepdims=True)

    def single(x):
        return [p.astype(f32) for p in pieces(x)]

    copies[0].wait()
    mean, square = moments(down_ref)
    for c in copies[1:4]:
        c.wait()
    scaled = (branch_scale * cotangent_ref[...].astype(f32)).astype(bf16)
    gain = single(gain_ref[...])
    left = jnp.concatenate([tokens_ref[...].astype(f32), *single(mean), gain[0]], axis=0).astype(bf16)
    right = jnp.concatenate([scaled.astype(f32), *single(square), gain[1]], axis=0).astype(bf16)
    wide = []
    for c, ref in zip(copies[4:], (gate_ref, up_ref)):
        c.wait()
        wide.append(moments(ref))
    blocks, lines = out_ref.shape[0], out_ref.shape[1]
    share = gate_ref.shape[1] // blocks
    for j in range(blocks):
        sides = []
        for side in range(2):
            parts = []
            for pair in wide:
                row = pair[side][:, j * share : (j + 1) * share]
                parts += single(jnp.concatenate([row, jnp.zeros((1, width - share), f32)], axis=1))
            sides.append(jnp.concatenate([*parts, jnp.zeros((2, width), f32)], axis=0).astype(bf16))
        for l in range(lines):
            out_ref[j, l, 0 : rows + 4, 0:width] = left
            out_ref[j, l, 0 : rows + 4, width : 2 * width] = right
            out_ref[j, l, rows + 4 : rows + 12, 0:width] = sides[0]
            out_ref[j, l, rows + 4 : rows + 12, width : 2 * width] = sides[1]


def pack_weights(place_ref, gate_hbm, up_hbm, down_hbm, *refs):
    *outs, store_ref, gate_ref, up_ref, down_ref, sems = refs
    copies = fetched(((gate_hbm, gate_ref), (up_hbm, up_ref), (down_hbm, down_ref)), sems)
    blocks, _, share, _ = store_ref.shape
    for at, ref in enumerate((gate_ref, up_ref)):
        copies[at].wait()
        turned = ref[...].astype(f32).T.astype(bf16)
        for j in range(blocks):
            store_ref[j, at] = turned[j * share : (j + 1) * share]
    copies[2].wait()
    for j in range(blocks):
        store_ref[j, 2] = down_ref[j * share : (j + 1) * share]
    for k in range(blocks):
        outs[k][...] = store_ref[lax.rem(place_ref[1] + k, blocks)]


def repack_tokens(wide_count, tall_count, place_ref, in_ref, out_ref, moment_ref):
    blocks, lines, high, wide = in_ref.shape
    rows = high - 12
    width = wide // 2
    for j in range(blocks):
        source = lax.rem(place_ref[1] + blocks - j, blocks)
        lots = [in_ref[source, l, 0 : rows + 4, :].astype(f32) for l in range(lines)]
        moments = [
            (joined(lot[rows : rows + 3, 0:width]), joined(lot[rows : rows + 3, width:])) for lot in lots
        ]
        mean, square = merged(moments, tall_count)
        zero = jnp.zeros((4, width), f32)
        for extra, a in ((mean, 0), (square, width)):
            parts = [lot[0:rows, a : a + width] for lot in lots]
            parts += [p.astype(f32) for p in pieces(extra)]
            parts += [lots[0][rows + 3 : rows + 4, a : a + width], zero]
            block = jnp.concatenate(parts, axis=0).astype(bf16)
            for y in range(out_ref.shape[0]):
                out_ref[y, j, :, a : a + width] = block
    line = place_ref[2]
    own = [in_ref[j, line, rows + 4 : rows + 12, :].astype(f32) for j in range(blocks)]
    found = []
    for at in range(2):
        moments = [
            (joined(o[3 * at : 3 * at + 3, 0:width]), joined(o[3 * at : 3 * at + 3, width:])) for o in own
        ]
        found += merged(moments, wide_count)
    block = jnp.concatenate([*found, jnp.zeros((4, width), f32)], axis=0)
    moment_ref[...] = block


def whole(own_ref, other_ref, j, at):
    rows = own_ref.shape[2] - 8
    width = own_ref.shape[3] // 2
    halves = [
        ref[:, j, 0:rows, at * width : (at + 1) * width].reshape(-1, width) for ref in (own_ref, other_ref)
    ]
    return jnp.concatenate(halves, axis=0)


def forward(
    wide_count, tall_count, place_ref, w0_ref, w1_ref, w2_ref, w3_ref, own_ref, other_ref,
    moment0_ref, moment1_ref, moment2_ref, moment3_ref, gate_gain_ref, up_gain_ref,
    kept_ref, first_ref, second_ref, third_ref,
    cols_ref, rows_ref, row_ref, store_ref,
):
    w_ref = (w0_ref, w1_ref, w2_ref, w3_ref)
    blocks = len(w_ref)
    _, share, width = w0_ref.shape
    parts = store_ref.shape[0]
    tall = share // parts
    lane = lax.broadcasted_iota(jnp.int32, cols_ref.shape, 1)
    cols = jnp.zeros(cols_ref.shape, f32)
    row = 0.0
    lefts = [whole(own_ref, other_ref, j, 0) for j in range(blocks)]
    ones = jnp.ones((8, width), bf16)
    for j in range(blocks):
        row = row + nt(ones, lefts[j])
    row_ref[...] = row
    for at in range(2):
        moments = [
            (ref[2 * at : 2 * at + 1, :], ref[2 * at + 1 : 2 * at + 2, :])
            for ref in (moment0_ref, moment1_ref, moment2_ref, moment3_ref)
        ]
        mean, square = merged(moments, wide_count)
        mean = upright(mean, share)
        scale = upright(lax.rsqrt(square + epsilon), share)
        row_of = (gate_gain_ref, up_gain_ref)[at]
        gain = sum(
            jnp.where(place_ref[1] == j, row_of[:, j * share : (j + 1) * share], 0.0) for j in range(blocks)
        )
        gain = upright(gain, share)
        gs = gain * scale
        for k, v in ((3 * at, mean), (3 * at + 1, gs), (3 * at + 2, scale), (6 + at, gain)):
            cols = jnp.where(lane == k, v, cols)
        total = 0.0
        for j in range(blocks):
            total = total + nt(w_ref[j][at], lefts[j])
        total = ((total - mean * row[0:1]) * gs).astype(bf16)
        for q in range(parts):
            store_ref[q, at * tall : (at + 1) * tall, :] = total[q * tall : (q + 1) * tall]
    cols_ref[...] = cols
    total = 0.0
    rows = own_ref.shape[2] - 8
    for j in range(blocks):
        lots = [
            ref[y, j, rows : rows + 8, :].astype(f32) for ref in (own_ref, other_ref) for y in range(own_ref.shape[0])
        ]
        mean, square = merged([(joined(lot[:, 0:width]), joined(lot[:, width:])) for lot in lots], tall_count)
        scale = lax.rsqrt(square + epsilon)
        gain = lots[0][3:4, 0:width] + lots[0][3:4, width:]
        gs = gain * scale
        rows_ref[j] = jnp.concatenate([mean, gs, scale, jnp.zeros((5, width), f32)], axis=0)
        hat = ((w_ref[j][2].astype(f32) - mean) * gs).astype(bf16)
        total = total + nt(hat, whole(own_ref, other_ref, j, 1))
    total = total.astype(bf16)
    for q in range(parts):
        store_ref[q, 2 * tall : 3 * tall, :] = total[q * tall : (q + 1) * tall]
    at, core = place_ref[0], place_ref[4]
    for ref, k in ((kept_ref, 0), (first_ref, 2), (second_ref, 3 - 2 * core), (third_ref, 1 + 2 * core)):
        ref[...] = store_ref[lax.rem(at + k, parts)]


def add_pair(a_ref, b_ref, out_ref):
    out_ref[...] = (a_ref[...].astype(f32) + b_ref[...].astype(f32)).astype(bf16)


def gating(kept_ref, second_ref, third_ref, row_ref, d_ref):
    tall = (d_ref.shape[0] - 8) // 3
    total = kept_ref[...].astype(f32) + second_ref[...].astype(f32) + third_ref[...].astype(f32)
    gate, up, dhidden = total[0:tall], total[tall : 2 * tall], total[2 * tall : 3 * tall]
    sig = 1.0 / (1.0 + jnp.exp(-gate))
    act = gate * sig
    d_gate = (dhidden * up * sig * (1.0 + gate * (1.0 - sig))).astype(bf16)
    d_up = (dhidden * act).astype(bf16)
    d_ref[2 * tall : 3 * tall, :] = (act * up).astype(bf16)
    d_ref[0:tall, :] = d_gate
    d_ref[tall : 2 * tall, :] = d_up
    dots = [
        level(jnp.sum(d.astype(f32) * v, axis=1, keepdims=True), 128)
        for d, v in ((d_gate, gate), (d_up, up))
    ]
    wide = d_ref.shape[1]
    dots = jnp.concatenate([*dots, jnp.zeros((1, wide - 256), f32)], axis=1)
    extra = [*pieces(dots), *pieces(row_ref[0:1, :])]
    extra = [p.astype(f32) for p in extra] + [jnp.zeros((2, wide), f32)]
    d_ref[3 * tall : 3 * tall + 8, :] = jnp.concatenate(extra, axis=0).astype(bf16)


def stacked(d_ref, at, tall):
    return jnp.concatenate(
        [d_ref[q, at * tall : (at + 1) * tall, :] for q in range(d_ref.shape[0])], axis=0
    )


def weight_grads(
    width_all, d_ref, w0_ref, w1_ref, w2_ref, w3_ref, own_ref, other_ref, cols_ref,
    g0_ref, g1_ref, g2_ref, g3_ref, dots_ref,
):
    w_ref = (w0_ref, w1_ref, w2_ref, w3_ref)
    blocks = len(w_ref)
    _, share, _ = w0_ref.shape
    grad_ref = (g0_ref, g1_ref, g2_ref, g3_ref)
    parts = d_ref.shape[0]
    tall = share // parts
    streams = [stacked(d_ref, at, tall) for at in range(3)]
    extra = [d_ref[q, 3 * tall : 3 * tall + 8, :].astype(f32) for q in range(parts)]
    row = sum(joined(e[3:6]) for e in extra)
    dots_ref[...] = jnp.zeros(dots_ref.shape, f32)
    means, pulls = [], []
    for at in range(2):
        means.append(jnp.sum(streams[at].astype(f32) * row, axis=1, keepdims=True) * (1.0 / width_all))
        dot = jnp.concatenate(
            [upright(joined(e[0:3, 128 * at : 128 * (at + 1)]), tall) for e in extra], axis=0
        )
        dots_ref[at : at + 1, :] = level(dot / cols_ref[:, 6 + at : 7 + at], dots_ref.shape[1])
        s = cols_ref[:, 3 * at + 2 : 3 * at + 3]
        pulls.append(s * s * dot)
    for j in range(blocks):
        left = whole(own_ref, other_ref, j, 0)
        for at in range(2):
            p = nn(streams[at], left)
            cent = w_ref[j][at].astype(f32) - cols_ref[:, 3 * at : 3 * at + 1]
            grad = cols_ref[:, 3 * at + 1 : 3 * at + 2] * (p - means[at]) - cent * pulls[at]
            grad_ref[j][at] = grad.astype(bf16)
        grad_ref[j][2] = nn(streams[2], whole(own_ref, other_ref, j, 1)).astype(bf16)


def spread(sums):
    return [p.astype(f32) for k in range(2) for p in pieces(sums[k : k + 1, :])]


def token_back(
    d_ref, w0_ref, w1_ref, w2_ref, w3_ref, own_ref, other_ref, cols_ref, rows_ref, mine_ref, theirs_ref, sums_ref
):
    w_ref = (w0_ref, w1_ref, w2_ref, w3_ref)
    blocks = len(w_ref)
    _, share, width = w0_ref.shape
    tall = share // d_ref.shape[0]
    streams = [stacked(d_ref, at, tall).T for at in range(2)]
    hidden = stacked(d_ref, 2, tall)
    half = mine_ref.shape[1]
    for j in range(blocks):
        back = 0.0
        for at in range(2):
            cent = w_ref[j][at].astype(f32) - cols_ref[:, 3 * at : 3 * at + 1]
            back = back + nn(streams[at], (cent * cols_ref[:, 3 * at + 1 : 3 * at + 2]).astype(bf16))
        mine_ref[j] = back[:half]
        p = nn(hidden, whole(own_ref, other_ref, j, 1))
        cent = w_ref[j][2].astype(f32) - rows_ref[j, 0:1, :]
        summed = jnp.sum(p, axis=0, keepdims=True)
        crossed = jnp.sum(p * cent, axis=0, keepdims=True)
        zero = jnp.zeros((6, width), f32)
        sums = jnp.concatenate([summed, crossed, zero], axis=0)
        sums_ref[j] = sums
        sums = jnp.concatenate([*spread(sums), zero[0:2]], axis=0)
        theirs_ref[j] = jnp.concatenate([back[half:], sums], axis=0).astype(bf16)


def both_cores(mine_ref, theirs_ref, sums_ref, out_ref):
    blocks, half, _ = mine_ref.shape
    lines = out_ref.shape[0]
    rows = half // lines
    for j in range(blocks):
        other = theirs_ref[j, half : half + 8, :].astype(f32)
        total = sums_ref[j, 0:2, :] + jnp.concatenate([joined(other[0:3]), joined(other[3:6])], axis=0)
        extra = jnp.concatenate([*spread(total), other[6:8]], axis=0).astype(bf16)
        for k in range(lines):
            at = slice(k * rows, (k + 1) * rows)
            out_ref[k, j, 0:rows, :] = (mine_ref[j, at, :] + theirs_ref[j, at, :].astype(f32)).astype(bf16)
            out_ref[k, j, rows : rows + 8, :] = extra


def whole_column(place_ref, in_ref, dots_ref, out_ref):
    lines, blocks, high, _ = in_ref.shape
    dots = spread(dots_ref[...])
    cuts = out_ref.shape[0]
    rows = (high - 8) // cuts
    for j in range(blocks):
        lots = [in_ref[y, j].astype(f32) for y in range(lines)]
        back = sum(lot[0 : high - 8] for lot in lots)
        total = [sum(joined(lot[high - 8 + 3 * k : high - 5 + 3 * k]) for lot in lots) for k in range(2)]
        extra = spread(jnp.concatenate(total, axis=0))
        for l in range(cuts):
            out_ref[l, lax.rem(place_ref[1] + blocks - j, blocks)] = jnp.concatenate(
                [back[l * rows : (l + 1) * rows], *extra, *dots], axis=0
            ).astype(bf16)


def finish_wide(place_ref, g0_ref, g1_ref, g2_ref, g3_ref, gate_ref, up_ref, store_ref):
    g_ref = (g0_ref, g1_ref, g2_ref, g3_ref)
    for at, ref in enumerate((gate_ref, up_ref)):
        for k, g in enumerate(g_ref):
            store_ref[lax.rem(place_ref[1] + k, len(g_ref))] = g[at].astype(f32)
        ref[...] = store_ref[...].reshape(-1, store_ref.shape[2]).T


def finish_tall(
    hidden_all, place_ref, in_ref, cotangent_ref, g0_ref, g1_ref, g2_ref, g3_ref, down_ref, rows_ref, gain_ref,
    tokens_ref, grad_ref, dgain_ref, dots_ref,
):
    lines, blocks, _, _ = in_ref.shape
    rows = tokens_ref.shape[0]
    lots = [in_ref[l, j].astype(f32) for l in range(lines) for j in range(blocks)]
    total = sum(lots)
    tokens_ref[...] = cotangent_ref[...].astype(f32) + total[0:rows]
    summed, crossed = (sum(joined(lot[rows + 3 * k : rows + 3 * k + 3]) for lot in lots) for k in range(2))
    line = place_ref[2]
    for j in range(blocks):
        own = in_ref[line, j].astype(f32)
        dots_ref[0:1, j, :] = joined(own[rows + 6 : rows + 9])
        dots_ref[1:2, j, :] = joined(own[rows + 9 : rows + 12])
    mine = rows_ref[0]
    mean, scale = mine[0:1, :], mine[2:3, :]
    gain = gain_ref[...]
    dgain_ref[...] = scale * crossed
    g_ref = (g0_ref, g1_ref, g2_ref, g3_ref)
    for k, g in enumerate(g_ref):
        j = lax.rem(place_ref[1] + k, len(g_ref))
        cent = down_ref[j].astype(f32) - mean
        grad_ref[j] = scale * gain * (g[2].astype(f32) - summed * (1.0 / hidden_all)) - (
            scale * scale * scale * gain * crossed
        ) * cent


def call(body, outs, *args, place=None, scratch=(), far=0, grant=20):
    specs = [pl.BlockSpec(memory_space=pltpu.HBM if i < far else pltpu.VMEM) for i in range(len(args))]
    if place is not None:
        args = (place, *args)
        specs = [pl.BlockSpec(memory_space=pltpu.SMEM), *specs]
    return pl.pallas_call(
        body,
        out_shape=[jax.ShapeDtypeStruct(s, t) for s, t in outs],
        in_specs=specs,
        scratch_shapes=scratch,
        compiler_params=pltpu.CompilerParams(vmem_limit_bytes=grant << 20),
    )(*args)


def exchange(x, axis):
    return lax.all_to_all(x, axis, split_axis=0, concat_axis=0, tiled=True)


def shift(x, axis, by):
    size = lax.axis_size(axis)
    return lax.ppermute(x, axis, [(i, (i + by) % size) for i in range(size)])


def apart(x, axis, by):
    size = lax.axis_size(axis)
    pairs = [
        (core * size + i, core * size + (i + (by if core == 0 else -by)) % size) for core in (0, 1) for i in range(size)
    ]
    return lax.ppermute(x, ("core", axis), pairs)


def block(tokens, cotangent, gate_weight, up_weight, down_weight, gate_gain, up_gain, down_gain):
    rows, width = tokens.shape
    hidden = gate_weight.shape[1]
    nx, nz, ny = lax.axis_size("x"), lax.axis_size("zh"), lax.axis_size("y")
    nl, nc = lax.axis_size("zl"), lax.axis_size("core")
    width_all = width * nx * nz
    hidden_all = hidden * ny * nl * nc
    share = hidden // nx
    tall = share // nz
    count = rows * ny * nl * nc
    place = jnp.stack(
        [lax.axis_index("zh"), lax.axis_index("x"), lax.axis_index("zl"), lax.axis_index("y"), lax.axis_index("core")]
    ).astype(jnp.int32)
    swap = [(0, 1), (1, 0)]

    def grid_exchange(x, axes):
        flat = exchange(x.reshape(x.shape[0] * x.shape[1], *x.shape[2:]), axes)
        return flat.reshape(x.shape)

    (both,) = call(
        pack_tokens, [((nx, nl, rows + 12, 2 * width), bf16)],
        down_weight, down_gain.reshape(1, width), tokens, cotangent, gate_weight, up_weight,
        far=6,
        grant=60,
        scratch=[
            pltpu.VMEM((hidden, width), bf16), pltpu.VMEM((1, width), f32),
            pltpu.VMEM((rows, width), bf16), pltpu.VMEM((rows, width), bf16),
            pltpu.VMEM((width, hidden), bf16), pltpu.VMEM((width, hidden), bf16), pltpu.SemaphoreType.DMA((6,)),
        ],
    )
    both = grid_exchange(both, ("x", "zl"))
    cut_weights = call(
        pack_weights, [((3, share, width), bf16)] * nx, gate_weight, up_weight, down_weight,
        place=place,
        far=3,
        scratch=[
            pltpu.VMEM((nx, 3, share, width), bf16),
            pltpu.VMEM((width, hidden), bf16), pltpu.VMEM((width, hidden), bf16), pltpu.VMEM((hidden, width), bf16),
            pltpu.SemaphoreType.DMA((3,)),
        ],
    )
    weights = [cut_weights[0]]
    for k in (1, 2, 3):
        weights.append(shift(cut_weights[k], "x", k))
    both, moments = call(
        functools.partial(repack_tokens, width, hidden),
        [((ny, nx, nl * rows + 8, 2 * width), bf16), ((8, width), f32)], both, place=place,
    )
    own = exchange(both, "y")
    moments = [moments, *(shift(moments, "zh", k) for k in (1, 2, 3))]
    other = lax.ppermute(own, "core", swap)
    piece = ((3 * tall, count), bf16)
    kept, first, second, third, cols, rows_of, row = call(
        functools.partial(forward, width * nx, hidden * nl),
        [piece, piece, piece, piece, ((share, 128), f32), ((nx, 8, width), f32), ((8, count), f32)],
        *weights, own, other, *moments, gate_gain.reshape(1, hidden), up_gain.reshape(1, hidden),
        place=place,
        scratch=[pltpu.VMEM((nz, 3 * tall, count), bf16)],
    )
    first = apart(first, "zh", 1)
    second = apart(second, "zh", -1)
    (third,) = call(add_pair, [piece], third, first)
    third = apart(third, "zh", 1)
    (d,) = call(gating, [((3 * tall + 8, count), bf16)], kept, second, third, row)
    d = lax.all_gather(d, "zh")

    half = count // nc
    mine, theirs, sums = call(
        token_back, [((nx, half, width), f32), ((nx, half + 8, width), bf16), ((nx, 8, width), f32)],
        d, *weights, own, other, cols, rows_of,
    )
    theirs = lax.ppermute(theirs, "core", swap)
    *grads, dots = call(
        functools.partial(weight_grads, width_all), [((3, share, width), bf16)] * nx + [((8, width), f32)],
        d, *weights, own, other, cols,
    )
    (back,) = call(both_cores, [((ny, nx, nl * rows + 8, width), bf16)], mine, theirs, sums)
    back = exchange(back, "y")
    sent = [grads[0], None, None, None]
    for k in (2, 1, 3):
        sent[k] = shift(grads[k], "x", -k)
    (back,) = call(whole_column, [((nl, nx, rows + 12, width), bf16)], back, dots, place=place)
    back = grid_exchange(back, ("zl", "x"))
    grad_gate, grad_up = call(finish_wide, [((width, hidden), f32), ((width, hidden), f32)], *sent,
        place=place, scratch=[pltpu.VMEM((nx, share, width), f32)],
    )
    grad_tokens, grad_down, down_dgain, dots = call(
        functools.partial(finish_tall, hidden_all),
        [((rows, width), f32), ((nx, share, width), f32), ((1, width), f32), ((2, nx, width), f32)],
        back, cotangent, *sent, down_weight.reshape(nx, share, width), rows_of, down_gain.reshape(1, width),
        place=place,
    )
    dots = dots[:, :, :share].reshape(2, hidden)
    return (
        grad_tokens,
        grad_gate,
        grad_up,
        grad_down.reshape(hidden, width),
        dots[0],
        dots[1],
        down_dgain.reshape(width),
    )


def solution(mesh):
    fine = Mesh(mesh.devices.reshape(4, 4, 2, 4, 4), (*BLK, *REP))
    return jax.shard_map(
        block,
        mesh=fine,
        in_specs=(
            P(BLK, REP), P(BLK, REP), P(REP, BLK), P(REP, BLK), P(BLK, REP), P(BLK), P(BLK), P(REP),
        ),
        out_specs=(
            P(BLK, REP), P(REP, BLK), P(REP, BLK), P(BLK, REP), P(BLK), P(BLK), P(REP),
        ),
        check_vma=False,
    )
```

```python
import functools

import jax
import jax.numpy as jnp
from jax import lax
from jax.experimental import pallas as pl
from jax.experimental.pallas import tpu as pltpu
from jax.sharding import Mesh, PartitionSpec as P


epsilon = 0.0001
branch_scale = 0.5
bf16 = jnp.bfloat16
f32 = jnp.float32

BLK = ("y", "zl", "core")
REP = ("zh", "x")


def nn(a, b):
    return lax.dot_general(a, b, (((1,), (0,)), ((), ())), preferred_element_type=f32)


def nt(a, b):
    return lax.dot_general(a, b, (((1,), (1,)), ((), ())), preferred_element_type=f32)


def pieces(x):
    high = x.astype(bf16)
    rest = x - high.astype(f32)
    middle = rest.astype(bf16)
    return high, middle, (rest - middle.astype(f32)).astype(bf16)


def joined(rows):
    return rows[0:1].astype(f32) + rows[1:2].astype(f32) + rows[2:3].astype(f32)


def merged(moments, count):
    mean = sum(m for m, _ in moments) * (1.0 / len(moments))
    square = sum(s for _, s in moments)
    for m, _ in moments:
        square = square + count * ((m - mean) * (m - mean))
    return mean, square


def upright(row, tall):
    shape = (tall, row.shape[1])
    same = lax.broadcasted_iota(jnp.int32, shape, 0) == lax.broadcasted_iota(jnp.int32, shape, 1)
    return jnp.sum(jnp.where(same, row, 0.0), axis=1, keepdims=True)


def level(col, wide):
    shape = (col.shape[0], wide)
    same = lax.broadcasted_iota(jnp.int32, shape, 0) == lax.broadcasted_iota(jnp.int32, shape, 1)
    return jnp.sum(jnp.where(same, col, 0.0), axis=0, keepdims=True)


def fetched(pairs, sems):
    copies = [pltpu.make_async_copy(a, b, sems.at[i]) for i, (a, b) in enumerate(pairs)]
    for c in copies:
        c.start()
    return copies


def pack_tokens(
    down_hbm, gain_hbm, tokens_hbm, cotangent_hbm, out_ref, down_ref, gain_ref, tokens_ref, cotangent_ref, sems
):
    copies = fetched(
        ((down_hbm, down_ref), (gain_hbm, gain_ref), (tokens_hbm, tokens_ref), (cotangent_hbm, cotangent_ref)), sems
    )
    _, width = tokens_ref.shape
    copies[0].wait()
    w = down_ref[...].astype(f32)
    mean = jnp.sum(w, axis=0, keepdims=True) * (1.0 / w.shape[0])
    off = w - mean
    square = jnp.sum(off * off, axis=0, keepdims=True)
    for c in copies[1:]:
        c.wait()
    scaled = (branch_scale * cotangent_ref[...].astype(f32)).astype(bf16)
    gain = pieces(gain_ref[...])
    left = [tokens_ref[...], *pieces(mean), gain[0]]
    right = [scaled, *pieces(square), gain[1]]
    for side, parts in enumerate((left, right)):
        block = jnp.concatenate([p.astype(f32) for p in parts], axis=0).astype(bf16)
        for j in range(out_ref.shape[0]):
            for l in range(out_ref.shape[1]):
                out_ref[j, l, :, side * width : (side + 1) * width] = block


def pack_weights(place_ref, gate_hbm, up_hbm, down_hbm, *refs):
    *outs, store_ref, gate_ref, up_ref, down_ref, sems = refs
    copies = fetched(((gate_hbm, gate_ref), (up_hbm, up_ref), (down_hbm, down_ref)), sems)
    blocks, _, share, _ = store_ref.shape
    for at, ref in enumerate((gate_ref, up_ref)):
        copies[at].wait()
        turned = ref[...].astype(f32).T.astype(bf16)
        for j in range(blocks):
            store_ref[j, at] = turned[j * share : (j + 1) * share]
    copies[2].wait()
    for j in range(blocks):
        store_ref[j, 2] = down_ref[j * share : (j + 1) * share]
    for k in range(blocks):
        outs[k][...] = store_ref[lax.rem(place_ref[1] + k, blocks)]


def repack_tokens(tall_count, place_ref, in_ref, out_ref):
    blocks, lines, high, wide = in_ref.shape
    rows = high - 4
    width = wide // 2
    for j in range(blocks):
        source = lax.rem(place_ref[1] + blocks - j, blocks)
        lots = [in_ref[source, l, 0 : rows + 4, :].astype(f32) for l in range(lines)]
        moments = [
            (joined(lot[rows : rows + 3, 0:width]), joined(lot[rows : rows + 3, width:])) for lot in lots
        ]
        mean, square = merged(moments, tall_count)
        zero = jnp.zeros((4, width), f32)
        for extra, a in ((mean, 0), (square, width)):
            parts = [lot[0:rows, a : a + width] for lot in lots]
            parts += [p.astype(f32) for p in pieces(extra)]
            parts += [lots[0][rows + 3 : rows + 4, a : a + width], zero]
            block = jnp.concatenate(parts, axis=0).astype(bf16)
            for y in range(out_ref.shape[0]):
                out_ref[y, j, :, a : a + width] = block


def whole(own_ref, other_ref, j, at):
    rows = own_ref.shape[2] - 8
    width = own_ref.shape[3] // 2
    halves = [
        ref[:, j, 0:rows, at * width : (at + 1) * width].reshape(-1, width) for ref in (own_ref, other_ref)
    ]
    return jnp.concatenate(halves, axis=0)


def moments_of(w_ref, at):
    blocks = [w[at].astype(f32) for w in w_ref]
    mean = sum(jnp.sum(w, axis=1, keepdims=True) for w in blocks) * (1.0 / (len(blocks) * blocks[0].shape[1]))
    square = sum(jnp.sum((w - mean) * (w - mean), axis=1, keepdims=True) for w in blocks)
    return mean, square


def forward(
    tall_count, place_ref, w0_ref, w1_ref, w2_ref, w3_ref, own_ref, other_ref,
    kept_ref, first_ref, second_ref, third_ref, rows_ref, news_ref, store_ref,
):
    w_ref = (w0_ref, w1_ref, w2_ref, w3_ref)
    blocks = len(w_ref)
    _, share, width = w0_ref.shape
    parts = store_ref.shape[0]
    tall = share // parts
    lefts = [whole(own_ref, other_ref, j, 0) for j in range(blocks)]
    ones = jnp.ones((8, width), bf16)
    row = sum(nt(ones, left) for left in lefts)[0:1]
    levels = []
    for at in range(2):
        mean, square = moments_of(w_ref, at)
        levels += [level(mean, 256), level(square, 256)]
        total = sum(nt(w_ref[j][at], lefts[j]) for j in range(blocks))
        total = (total - mean * row).astype(bf16)
        for q in range(parts):
            store_ref[q, at * tall : (at + 1) * tall, :] = total[q * tall : (q + 1) * tall]
    rest = jnp.zeros((1, row.shape[1] - 512), f32)
    lines = [row] + [jnp.concatenate([levels[2 * at], levels[2 * at + 1], rest], axis=1) for at in range(2)]
    lines = [p.astype(f32) for line in lines for p in pieces(line)[0:2]]
    news_ref[...] = jnp.concatenate([*lines, jnp.zeros((2, row.shape[1]), f32)], axis=0).astype(bf16)
    total = 0.0
    rows = own_ref.shape[2] - 8
    for j in range(blocks):
        lots = [
            ref[y, j, rows : rows + 8, :].astype(f32) for ref in (own_ref, other_ref) for y in range(own_ref.shape[0])
        ]
        mean, square = merged([(joined(lot[:, 0:width]), joined(lot[:, width:])) for lot in lots], tall_count)
        scale = lax.rsqrt(square + epsilon)
        gain = lots[0][3:4, 0:width] + lots[0][3:4, width:]
        gs = gain * scale
        rows_ref[j] = jnp.concatenate([mean, gs, scale, jnp.zeros((5, width), f32)], axis=0)
        hat = ((w_ref[j][2].astype(f32) - mean) * gs).astype(bf16)
        total = total + nt(hat, whole(own_ref, other_ref, j, 1))
    total = total.astype(bf16)
    for q in range(parts):
        store_ref[q, 2 * tall : 3 * tall, :] = total[q * tall : (q + 1) * tall]
    at, core = place_ref[0], place_ref[4]
    for ref, k in ((kept_ref, 0), (first_ref, 2), (second_ref, 3 - 2 * core), (third_ref, 1 + 2 * core)):
        ref[0 : 3 * tall, :] = store_ref[lax.rem(at + k, parts)]
    for ref in (first_ref, second_ref):
        ref[3 * tall : 3 * tall + 8, :] = news_ref[...]


def add_pair(a_ref, b_ref, out_ref):
    high = a_ref.shape[0]
    out_ref[0:high, :] = (a_ref[...].astype(f32) + b_ref[0:high, :].astype(f32)).astype(bf16)
    out_ref[high:, :] = b_ref[high:, :]


def gating(
    wide_count, place_ref, kept_ref, first_ref, second_ref, third_ref, news_ref, gate_gain_ref, up_gain_ref,
    d_ref, cols_ref, row_ref,
):
    tall = (d_ref.shape[0] - 8) // 3
    share = cols_ref.shape[0]
    high = 3 * tall
    news = [news_ref[...].astype(f32)]
    news += [ref[high : high + 8, :].astype(f32) for ref in (first_ref, second_ref, third_ref)]
    rows = [n[0:1] + n[1:2] for n in news]
    row = sum(rows)
    row_ref[...] = jnp.broadcast_to(row, row_ref.shape)
    lane = lax.broadcasted_iota(jnp.int32, cols_ref.shape, 1)
    cols = jnp.zeros(cols_ref.shape, f32)
    for at in range(2):
        both = [n[2 * at + 2 : 2 * at + 3] + n[2 * at + 3 : 2 * at + 4] for n in news]
        moments = [(b[:, 0:256], b[:, 256:512]) for b in both]
        mean, square = merged(moments, wide_count)
        gains = (gate_gain_ref, up_gain_ref)[at]
        gain = sum(
            jnp.where(place_ref[1] == j, gains[:, j * share : (j + 1) * share], 0.0)
            for j in range(gains.shape[1] // share)
        )
        scale = upright(lax.rsqrt(square + epsilon), share)
        gain = upright(gain, share)
        found = [(3 * at, upright(mean, share)), (3 * at + 1, gain * scale), (3 * at + 2, scale), (6 + at, gain)]
        found += [(8 + 4 * at + q, upright(m, share)) for q, (m, _) in enumerate(moments)]
        for k, v in found:
            cols = jnp.where(lane == k, v, cols)
    cols_ref[...] = cols
    mine = cols_ref[pl.ds(pl.multiple_of(place_ref[0] * tall, 8), tall), :]
    total = kept_ref[...].astype(f32) + second_ref[0:high, :].astype(f32) + third_ref[0:high, :].astype(f32)
    sums = []
    for at in range(2):
        x = total[at * tall : (at + 1) * tall] - mine[:, 3 * at : 3 * at + 1] * row
        for q, r in enumerate(rows):
            x = x + mine[:, 8 + 4 * at + q : 9 + 4 * at + q] * r
        sums.append(mine[:, 3 * at + 1 : 3 * at + 2] * x)
    gate, up = sums
    dhidden = total[2 * tall : 3 * tall]
    sig = 1.0 / (1.0 + jnp.exp(-gate))
    act = gate * sig
    d_gate = (dhidden * up * sig * (1.0 + gate * (1.0 - sig))).astype(bf16)
    d_up = (dhidden * act).astype(bf16)
    d_ref[2 * tall : 3 * tall, :] = (act * up).astype(bf16)
    d_ref[0:tall, :] = d_gate
    d_ref[tall : 2 * tall, :] = d_up
    dots = [
        level(jnp.sum(d.astype(f32) * v, axis=1, keepdims=True), 128)
        for d, v in ((d_gate, gate), (d_up, up))
    ]
    wide = d_ref.shape[1]
    dots = jnp.concatenate([*dots, jnp.zeros((1, wide - 256), f32)], axis=1)
    extra = [p.astype(f32) for p in pieces(dots)] + [jnp.zeros((5, wide), f32)]
    d_ref[3 * tall : 3 * tall + 8, :] = jnp.concatenate(extra, axis=0).astype(bf16)


def stacked(d_ref, at, tall):
    return jnp.concatenate(
        [d_ref[q, at * tall : (at + 1) * tall, :] for q in range(d_ref.shape[0])], axis=0
    )


def weight_grads(
    width_all, d_ref, w0_ref, w1_ref, w2_ref, w3_ref, own_ref, other_ref, cols_ref, row_ref,
    g0_ref, g1_ref, g2_ref, g3_ref, dots_ref,
):
    w_ref = (w0_ref, w1_ref, w2_ref, w3_ref)
    blocks = len(w_ref)
    _, share, _ = w0_ref.shape
    grad_ref = (g0_ref, g1_ref, g2_ref, g3_ref)
    parts = d_ref.shape[0]
    tall = share // parts
    streams = [stacked(d_ref, at, tall) for at in range(3)]
    extra = [d_ref[q, 3 * tall : 3 * tall + 8, :].astype(f32) for q in range(parts)]
    row = row_ref[0:1, :]
    dots_ref[...] = jnp.zeros(dots_ref.shape, f32)
    means, pulls = [], []
    for at in range(2):
        means.append(jnp.sum(streams[at].astype(f32) * row, axis=1, keepdims=True) * (1.0 / width_all))
        dot = jnp.concatenate(
            [upright(joined(e[0:3, 128 * at : 128 * (at + 1)]), tall) for e in extra], axis=0
        )
        dots_ref[at : at + 1, :] = level(dot / cols_ref[:, 6 + at : 7 + at], dots_ref.shape[1])
        s = cols_ref[:, 3 * at + 2 : 3 * at + 3]
        pulls.append(s * s * dot)
    for j in range(blocks):
        left = whole(own_ref, other_ref, j, 0)
        for at in range(2):
            p = nn(streams[at], left)
            cent = w_ref[j][at].astype(f32) - cols_ref[:, 3 * at : 3 * at + 1]
            grad = cols_ref[:, 3 * at + 1 : 3 * at + 2] * (p - means[at]) - cent * pulls[at]
            grad_ref[j][at] = grad.astype(bf16)
        grad_ref[j][2] = nn(streams[2], whole(own_ref, other_ref, j, 1)).astype(bf16)


def spread(sums):
    return [p.astype(f32) for k in range(2) for p in pieces(sums[k : k + 1, :])]


def token_back(
    d_ref, w0_ref, w1_ref, w2_ref, w3_ref, own_ref, other_ref, cols_ref, rows_ref, mine_ref, theirs_ref, sums_ref
):
    w_ref = (w0_ref, w1_ref, w2_ref, w3_ref)
    blocks = len(w_ref)
    _, share, width = w0_ref.shape
    tall = share // d_ref.shape[0]
    streams = [stacked(d_ref, at, tall).T for at in range(2)]
    hidden = stacked(d_ref, 2, tall)
    half = mine_ref.shape[1]
    for j in range(blocks):
        back = 0.0
        for at in range(2):
            cent = w_ref[j][at].astype(f32) - cols_ref[:, 3 * at : 3 * at + 1]
            back = back + nn(streams[at], (cent * cols_ref[:, 3 * at + 1 : 3 * at + 2]).astype(bf16))
        mine_ref[j] = back[:half]
        p = nn(hidden, whole(own_ref, other_ref, j, 1))
        cent = w_ref[j][2].astype(f32) - rows_ref[j, 0:1, :]
        summed = jnp.sum(p, axis=0, keepdims=True)
        crossed = jnp.sum(p * cent, axis=0, keepdims=True)
        zero = jnp.zeros((6, width), f32)
        sums = jnp.concatenate([summed, crossed, zero], axis=0)
        sums_ref[j] = sums
        sums = jnp.concatenate([*spread(sums), zero[0:2]], axis=0)
        theirs_ref[j] = jnp.concatenate([back[half:], sums], axis=0).astype(bf16)


def both_cores(mine_ref, theirs_ref, sums_ref, out_ref):
    blocks, half, _ = mine_ref.shape
    lines = out_ref.shape[0]
    rows = half // lines
    for j in range(blocks):
        other = theirs_ref[j, half : half + 8, :].astype(f32)
        total = sums_ref[j, 0:2, :] + jnp.concatenate([joined(other[0:3]), joined(other[3:6])], axis=0)
        extra = jnp.concatenate([*spread(total), other[6:8]], axis=0).astype(bf16)
        for k in range(lines):
            at = slice(k * rows, (k + 1) * rows)
            out_ref[k, j, 0:rows, :] = (mine_ref[j, at, :] + theirs_ref[j, at, :].astype(f32)).astype(bf16)
            out_ref[k, j, rows : rows + 8, :] = extra


def whole_column(place_ref, in_ref, dots_ref, out_ref):
    lines, blocks, high, _ = in_ref.shape
    dots = spread(dots_ref[...])
    cuts = out_ref.shape[0]
    rows = (high - 8) // cuts
    for j in range(blocks):
        lots = [in_ref[y, j].astype(f32) for y in range(lines)]
        back = sum(lot[0 : high - 8] for lot in lots)
        total = [sum(joined(lot[high - 8 + 3 * k : high - 5 + 3 * k]) for lot in lots) for k in range(2)]
        extra = spread(jnp.concatenate(total, axis=0))
        for l in range(cuts):
            out_ref[l, lax.rem(place_ref[1] + blocks - j, blocks)] = jnp.concatenate(
                [back[l * rows : (l + 1) * rows], *extra, *dots], axis=0
            ).astype(bf16)


def finish_wide(place_ref, g0_ref, g1_ref, g2_ref, g3_ref, gate_ref, up_ref, store_ref):
    g_ref = (g0_ref, g1_ref, g2_ref, g3_ref)
    for at, ref in enumerate((gate_ref, up_ref)):
        for k, g in enumerate(g_ref):
            store_ref[lax.rem(place_ref[1] + k, len(g_ref))] = g[at].astype(f32)
        ref[...] = store_ref[...].reshape(-1, store_ref.shape[2]).T


def finish_tall(
    hidden_all, place_ref, in_ref, cotangent_ref, g0_ref, g1_ref, g2_ref, g3_ref, down_ref, rows_ref, gain_ref,
    tokens_ref, grad_ref, dgain_ref, dots_ref,
):
    lines, blocks, _, _ = in_ref.shape
    rows = tokens_ref.shape[0]
    lots = [in_ref[l, j].astype(f32) for l in range(lines) for j in range(blocks)]
    total = sum(lots)
    tokens_ref[...] = cotangent_ref[...].astype(f32) + total[0:rows]
    summed, crossed = (sum(joined(lot[rows + 3 * k : rows + 3 * k + 3]) for lot in lots) for k in range(2))
    line = place_ref[2]
    for j in range(blocks):
        own = in_ref[line, j].astype(f32)
        dots_ref[0:1, j, :] = joined(own[rows + 6 : rows + 9])
        dots_ref[1:2, j, :] = joined(own[rows + 9 : rows + 12])
    mine = rows_ref[0]
    mean, scale = mine[0:1, :], mine[2:3, :]
    gain = gain_ref[...]
    dgain_ref[...] = scale * crossed
    g_ref = (g0_ref, g1_ref, g2_ref, g3_ref)
    for k, g in enumerate(g_ref):
        j = lax.rem(place_ref[1] + k, len(g_ref))
        cent = down_ref[j].astype(f32) - mean
        grad_ref[j] = scale * gain * (g[2].astype(f32) - summed * (1.0 / hidden_all)) - (
            scale * scale * scale * gain * crossed
        ) * cent


def call(body, outs, *args, place=None, scratch=(), far=0, grant=20):
    specs = [pl.BlockSpec(memory_space=pltpu.HBM if i < far else pltpu.VMEM) for i in range(len(args))]
    if place is not None:
        args = (place, *args)
        specs = [pl.BlockSpec(memory_space=pltpu.SMEM), *specs]
    return pl.pallas_call(
        body,
        out_shape=[jax.ShapeDtypeStruct(s, t) for s, t in outs],
        in_specs=specs,
        scratch_shapes=scratch,
        compiler_params=pltpu.CompilerParams(vmem_limit_bytes=grant << 20),
    )(*args)


def exchange(x, axis):
    return lax.all_to_all(x, axis, split_axis=0, concat_axis=0, tiled=True)


def shift(x, axis, by):
    size = lax.axis_size(axis)
    return lax.ppermute(x, axis, [(i, (i + by) % size) for i in range(size)])


def apart(x, axis, by):
    size = lax.axis_size(axis)
    pairs = [
        (core * size + i, core * size + (i + (by if core == 0 else -by)) % size) for core in (0, 1) for i in range(size)
    ]
    return lax.ppermute(x, ("core", axis), pairs)


def block(tokens, cotangent, gate_weight, up_weight, down_weight, gate_gain, up_gain, down_gain):
    rows, width = tokens.shape
    hidden = gate_weight.shape[1]
    nx, nz, ny = lax.axis_size("x"), lax.axis_size("zh"), lax.axis_size("y")
    nl, nc = lax.axis_size("zl"), lax.axis_size("core")
    width_all = width * nx * nz
    hidden_all = hidden * ny * nl * nc
    share = hidden // nx
    tall = share // nz
    count = rows * ny * nl * nc
    place = jnp.stack(
        [lax.axis_index("zh"), lax.axis_index("x"), lax.axis_index("zl"), lax.axis_index("y"), lax.axis_index("core")]
    ).astype(jnp.int32)
    swap = [(0, 1), (1, 0)]

    def grid_exchange(x, axes):
        flat = exchange(x.reshape(x.shape[0] * x.shape[1], *x.shape[2:]), axes)
        return flat.reshape(x.shape)

    (both,) = call(
        pack_tokens, [((nx, nl, rows + 4, 2 * width), bf16)],
        down_weight, down_gain.reshape(1, width), tokens, cotangent,
        far=4,
        grant=60,
        scratch=[
            pltpu.VMEM((hidden, width), bf16), pltpu.VMEM((1, width), f32),
            pltpu.VMEM((rows, width), bf16), pltpu.VMEM((rows, width), bf16), pltpu.SemaphoreType.DMA((4,)),
        ],
    )
    both = grid_exchange(both, ("x", "zl"))
    cut_weights = call(
        pack_weights, [((3, share, width), bf16)] * nx, gate_weight, up_weight, down_weight,
        place=place,
        far=3,
        scratch=[
            pltpu.VMEM((nx, 3, share, width), bf16),
            pltpu.VMEM((width, hidden), bf16), pltpu.VMEM((width, hidden), bf16), pltpu.VMEM((hidden, width), bf16),
            pltpu.SemaphoreType.DMA((3,)),
        ],
    )
    weights = [cut_weights[0]]
    for k in (1, 2, 3):
        weights.append(shift(cut_weights[k], "x", k))
    (both,) = call(
        functools.partial(repack_tokens, hidden), [((ny, nx, nl * rows + 8, 2 * width), bf16)], both, place=place
    )
    own = exchange(both, "y")
    other = lax.ppermute(own, "core", swap)
    piece, sent = ((3 * tall, count), bf16), ((3 * tall + 8, count), bf16)
    kept, first, second, third, rows_of, news = call(
        functools.partial(forward, hidden * nl),
        [piece, sent, sent, piece, ((nx, 8, width), f32), ((8, count), bf16)],
        *weights, own, other,
        place=place,
        scratch=[pltpu.VMEM((nz, 3 * tall, count), bf16)],
    )
    first = apart(first, "zh", 1)
    second = apart(second, "zh", -1)
    (third,) = call(add_pair, [sent], third, first)
    third = apart(third, "zh", 1)
    d, cols, row = call(
        functools.partial(gating, width * nx),
        [((3 * tall + 8, count), bf16), ((share, 128), f32), ((8, count), f32)],
        kept, first, second, third, news, gate_gain.reshape(1, hidden), up_gain.reshape(1, hidden),
        place=place,
    )
    d = lax.all_gather(d, "zh")

    half = count // nc
    mine, theirs, sums = call(
        token_back, [((nx, half, width), f32), ((nx, half + 8, width), bf16), ((nx, 8, width), f32)],
        d, *weights, own, other, cols, rows_of,
    )
    theirs = lax.ppermute(theirs, "core", swap)
    *grads, dots = call(
        functools.partial(weight_grads, width_all), [((3, share, width), bf16)] * nx + [((8, width), f32)],
        d, *weights, own, other, cols, row,
    )
    (back,) = call(both_cores, [((ny, nx, nl * rows + 8, width), bf16)], mine, theirs, sums)
    back = exchange(back, "y")
    met = [grads[0], None, None, None]
    for k in (2, 1, 3):
        met[k] = shift(grads[k], "x", -k)
    (back,) = call(whole_column, [((nl, nx, rows + 12, width), bf16)], back, dots, place=place)
    back = grid_exchange(back, ("zl", "x"))
    grad_gate, grad_up = call(finish_wide, [((width, hidden), f32), ((width, hidden), f32)], *met,
        place=place, scratch=[pltpu.VMEM((nx, share, width), f32)],
    )
    grad_tokens, grad_down, down_dgain, dots = call(
        functools.partial(finish_tall, hidden_all),
        [((rows, width), f32), ((nx, share, width), f32), ((1, width), f32), ((2, nx, width), f32)],
        back, cotangent, *met, down_weight.reshape(nx, share, width), rows_of, down_gain.reshape(1, width),
        place=place,
    )
    dots = dots[:, :, :share].reshape(2, hidden)
    return (
        grad_tokens,
        grad_gate,
        grad_up,
        grad_down.reshape(hidden, width),
        dots[0],
        dots[1],
        down_dgain.reshape(width),
    )


def solution(mesh):
    fine = Mesh(mesh.devices.reshape(4, 4, 2, 4, 4), (*BLK, *REP))
    return jax.shard_map(
        block,
        mesh=fine,
        in_specs=(
            P(BLK, REP), P(BLK, REP), P(REP, BLK), P(REP, BLK), P(BLK, REP), P(BLK), P(BLK), P(REP),
        ),
        out_specs=(
            P(BLK, REP), P(REP, BLK), P(REP, BLK), P(BLK, REP), P(BLK), P(BLK), P(REP),
        ),
        check_vma=False,
    )
```

```python
import functools

import jax
import jax.numpy as jnp
from jax import lax
from jax.experimental import pallas as pl
from jax.experimental.pallas import tpu as pltpu
from jax.sharding import Mesh, PartitionSpec as P


epsilon = 0.0001
branch_scale = 0.5
bf16 = jnp.bfloat16
f32 = jnp.float32

BLK = ("y", "zl", "core")
REP = ("zh", "x")


def nn(a, b):
    return lax.dot_general(a, b, (((1,), (0,)), ((), ())), preferred_element_type=f32)


def nt(a, b):
    return lax.dot_general(a, b, (((1,), (1,)), ((), ())), preferred_element_type=f32)


def pieces(x):
    high = x.astype(bf16)
    rest = x - high.astype(f32)
    middle = rest.astype(bf16)
    return high, middle, (rest - middle.astype(f32)).astype(bf16)


def joined(rows):
    return rows[0:1].astype(f32) + rows[1:2].astype(f32) + rows[2:3].astype(f32)


def merged(moments, count):
    mean = sum(m for m, _ in moments) * (1.0 / len(moments))
    square = sum(s for _, s in moments)
    for m, _ in moments:
        square = square + count * ((m - mean) * (m - mean))
    return mean, square


def upright(row, tall):
    shape = (tall, row.shape[1])
    same = lax.broadcasted_iota(jnp.int32, shape, 0) == lax.broadcasted_iota(jnp.int32, shape, 1)
    return jnp.sum(jnp.where(same, row, 0.0), axis=1, keepdims=True)


def level(col, wide):
    shape = (col.shape[0], wide)
    same = lax.broadcasted_iota(jnp.int32, shape, 0) == lax.broadcasted_iota(jnp.int32, shape, 1)
    return jnp.sum(jnp.where(same, col, 0.0), axis=0, keepdims=True)


def fetched(pairs, sems):
    copies = [pltpu.make_async_copy(a, b, sems.at[i]) for i, (a, b) in enumerate(pairs)]
    for c in copies:
        c.start()
    return copies


def pack_tokens(
    down_hbm, gain_hbm, tokens_hbm, cotangent_hbm, out_ref, down_ref, gain_ref, tokens_ref, cotangent_ref, sems
):
    copies = fetched(
        ((down_hbm, down_ref), (gain_hbm, gain_ref), (tokens_hbm, tokens_ref), (cotangent_hbm, cotangent_ref)), sems
    )
    _, width = tokens_ref.shape
    copies[0].wait()
    w = down_ref[...].astype(f32)
    mean = jnp.sum(w, axis=0, keepdims=True) * (1.0 / w.shape[0])
    off = w - mean
    square = jnp.sum(off * off, axis=0, keepdims=True)
    for c in copies[1:]:
        c.wait()
    scaled = (branch_scale * cotangent_ref[...].astype(f32)).astype(bf16)
    gain = pieces(gain_ref[...])
    left = [tokens_ref[...], *pieces(mean), gain[0]]
    right = [scaled, *pieces(square), gain[1]]
    for side, parts in enumerate((left, right)):
        block = jnp.concatenate([p.astype(f32) for p in parts], axis=0).astype(bf16)
        for j in range(out_ref.shape[0]):
            for l in range(out_ref.shape[1]):
                out_ref[j, l, :, side * width : (side + 1) * width] = block


def pack_weights(place_ref, gate_hbm, up_hbm, down_hbm, *refs):
    *outs, store_ref, gate_ref, up_ref, down_ref, sems = refs
    copies = fetched(((gate_hbm, gate_ref), (up_hbm, up_ref), (down_hbm, down_ref)), sems)
    blocks, _, share, _ = store_ref.shape
    for at, ref in enumerate((gate_ref, up_ref)):
        copies[at].wait()
        turned = ref[...].astype(f32).T.astype(bf16)
        for j in range(blocks):
            store_ref[j, at] = turned[j * share : (j + 1) * share]
    copies[2].wait()
    for j in range(blocks):
        store_ref[j, 2] = down_ref[j * share : (j + 1) * share]
    for k in range(blocks):
        outs[k][...] = store_ref[lax.rem(place_ref[1] + k, blocks)]


def repack_tokens(tall_count, place_ref, in_ref, out_ref):
    blocks, lines, high, wide = in_ref.shape
    rows = high - 4
    width = wide // 2
    for j in range(blocks):
        source = lax.rem(place_ref[1] + blocks - j, blocks)
        lots = [in_ref[source, l, 0 : rows + 4, :].astype(f32) for l in range(lines)]
        moments = [
            (joined(lot[rows : rows + 3, 0:width]), joined(lot[rows : rows + 3, width:])) for lot in lots
        ]
        mean, square = merged(moments, tall_count)
        zero = jnp.zeros((4, width), f32)
        for extra, a in ((mean, 0), (square, width)):
            parts = [lot[0:rows, a : a + width] for lot in lots]
            parts += [p.astype(f32) for p in pieces(extra)]
            parts += [lots[0][rows + 3 : rows + 4, a : a + width], zero]
            block = jnp.concatenate(parts, axis=0).astype(bf16)
            for y in range(out_ref.shape[0]):
                out_ref[y, j, :, a : a + width] = block


def whole(token_refs, j, at):
    rows = token_refs[0].shape[2] - 8
    width = token_refs[0].shape[3] // 2
    halves = [ref[:, j, 0:rows, at * width : (at + 1) * width].reshape(-1, width) for ref in token_refs]
    return jnp.concatenate(halves, axis=0)


def moments_of(w_ref, at):
    blocks = [w[at].astype(f32) for w in w_ref]
    mean = sum(jnp.sum(w, axis=1, keepdims=True) for w in blocks) * (1.0 / (len(blocks) * blocks[0].shape[1]))
    square = sum(jnp.sum((w - mean) * (w - mean), axis=1, keepdims=True) for w in blocks)
    return mean, square


def forward(
    tall_count, place_ref, w0_ref, w1_ref, w2_ref, w3_ref, *refs
):
    token_refs = refs[:2]
    kept_ref, first_ref, second_ref, third_ref, rows_ref, news_ref, store_ref = refs[2:]
    w_ref = (w0_ref, w1_ref, w2_ref, w3_ref)
    blocks = len(w_ref)
    _, share, width = w0_ref.shape
    parts = store_ref.shape[0]
    tall = share // parts
    lefts = [whole(token_refs, j, 0) for j in range(blocks)]
    ones = jnp.ones((8, width), bf16)
    row = sum(nt(ones, left) for left in lefts)[0:1]
    levels = []
    for at in range(2):
        mean, square = moments_of(w_ref, at)
        levels += [level(mean, 256), level(square, 256)]
        total = sum(nt(w_ref[j][at], lefts[j]) for j in range(blocks))
        total = (total - mean * row).astype(bf16)
        for q in range(parts):
            store_ref[q, at * tall : (at + 1) * tall, :] = total[q * tall : (q + 1) * tall]
    rest = jnp.zeros((1, row.shape[1] - 512), f32)
    lines = [row] + [jnp.concatenate([levels[2 * at], levels[2 * at + 1], rest], axis=1) for at in range(2)]
    lines = [p.astype(f32) for line in lines for p in pieces(line)[0:2]]
    news_ref[...] = jnp.concatenate([*lines, jnp.zeros((2, row.shape[1]), f32)], axis=0).astype(bf16)
    total = 0.0
    rows = token_refs[0].shape[2] - 8
    for j in range(blocks):
        lots = [
            ref[y, j, rows : rows + 8, :].astype(f32) for ref in token_refs for y in range(token_refs[0].shape[0])
        ]
        mean, square = merged([(joined(lot[:, 0:width]), joined(lot[:, width:])) for lot in lots], tall_count)
        scale = lax.rsqrt(square + epsilon)
        gain = lots[0][3:4, 0:width] + lots[0][3:4, width:]
        gs = gain * scale
        rows_ref[j] = jnp.concatenate([mean, gs, scale, jnp.zeros((5, width), f32)], axis=0)
        hat = ((w_ref[j][2].astype(f32) - mean) * gs).astype(bf16)
        total = total + nt(hat, whole(token_refs, j, 1))
    total = total.astype(bf16)
    for q in range(parts):
        store_ref[q, 2 * tall : 3 * tall, :] = total[q * tall : (q + 1) * tall]
    at, core = place_ref[0], place_ref[4]
    for ref, k in ((kept_ref, 0), (first_ref, 2), (second_ref, 3 - 2 * core), (third_ref, 1 + 2 * core)):
        ref[0 : 3 * tall, :] = store_ref[lax.rem(at + k, parts)]
    for ref in (first_ref, second_ref):
        ref[3 * tall : 3 * tall + 8, :] = news_ref[...]


def add_pair(a_ref, b_ref, out_ref):
    high = a_ref.shape[0]
    out_ref[0:high, :] = (a_ref[...].astype(f32) + b_ref[0:high, :].astype(f32)).astype(bf16)
    out_ref[high:, :] = b_ref[high:, :]


def gating(
    wide_count, place_ref, kept_ref, first_ref, second_ref, third_ref, news_ref, gate_gain_ref, up_gain_ref,
    d_ref, cols_ref, row_ref,
):
    tall = (d_ref.shape[0] - 8) // 3
    share = cols_ref.shape[0]
    high = 3 * tall
    news = [news_ref[...].astype(f32)]
    news += [ref[high : high + 8, :].astype(f32) for ref in (first_ref, second_ref, third_ref)]
    rows = [n[0:1] + n[1:2] for n in news]
    row = sum(rows)
    row_ref[...] = jnp.broadcast_to(row, row_ref.shape)
    wide = 256
    lines = [None] * 16
    for at in range(2):
        both = [n[2 * at + 2 : 2 * at + 3] + n[2 * at + 3 : 2 * at + 4] for n in news]
        moments = [(b[:, 0:wide], b[:, wide : 2 * wide]) for b in both]
        mean, square = merged(moments, wide_count)
        gains = (gate_gain_ref, up_gain_ref)[at]
        gain = sum(
            jnp.where(place_ref[1] == j, gains[:, j * share : (j + 1) * share], 0.0)
            for j in range(gains.shape[1] // share)
        )
        gain = jnp.concatenate([gain, jnp.zeros((1, wide - share), f32)], axis=1)
        scale = lax.rsqrt(square + epsilon)
        lines[3 * at : 3 * at + 3] = [mean, gain * scale, scale]
        lines[6 + at] = gain
        lines[8 + 4 * at : 12 + 4 * at] = [m for m, _ in moments]
    lines.append(jnp.zeros((cols_ref.shape[1] - 16, wide), f32))
    cols_ref[...] = jnp.concatenate(lines, axis=0).T[0:share]
    mine = cols_ref[pl.ds(pl.multiple_of(place_ref[0] * tall, 8), tall), :]
    total = kept_ref[...].astype(f32) + second_ref[0:high, :].astype(f32) + third_ref[0:high, :].astype(f32)
    sums = []
    for at in range(2):
        x = total[at * tall : (at + 1) * tall] - mine[:, 3 * at : 3 * at + 1] * row
        for q, r in enumerate(rows):
            x = x + mine[:, 8 + 4 * at + q : 9 + 4 * at + q] * r
        sums.append(mine[:, 3 * at + 1 : 3 * at + 2] * x)
    gate, up = sums
    dhidden = total[2 * tall : 3 * tall]
    sig = 1.0 / (1.0 + jnp.exp(-gate))
    act = gate * sig
    d_gate = (dhidden * up * sig * (1.0 + gate * (1.0 - sig))).astype(bf16)
    d_up = (dhidden * act).astype(bf16)
    d_ref[2 * tall : 3 * tall, :] = (act * up).astype(bf16)
    d_ref[0:tall, :] = d_gate
    d_ref[tall : 2 * tall, :] = d_up
    dots = [
        level(jnp.sum(d.astype(f32) * v, axis=1, keepdims=True), 128)
        for d, v in ((d_gate, gate), (d_up, up))
    ]
    wide = d_ref.shape[1]
    dots = jnp.concatenate([*dots, jnp.zeros((1, wide - 256), f32)], axis=1)
    extra = [p.astype(f32) for p in pieces(dots)] + [jnp.zeros((5, wide), f32)]
    d_ref[3 * tall : 3 * tall + 8, :] = jnp.concatenate(extra, axis=0).astype(bf16)


def stacked(d_ref, at, tall):
    return jnp.concatenate(
        [d_ref[q, at * tall : (at + 1) * tall, :] for q in range(d_ref.shape[0])], axis=0
    )


def weight_grads(width_all, d_ref, w0_ref, w1_ref, w2_ref, w3_ref, *refs):
    token_refs = refs[:2]
    cols_ref, row_ref, *grad_ref = refs[2:]
    w_ref = (w0_ref, w1_ref, w2_ref, w3_ref)
    blocks = len(w_ref)
    _, share, width = w0_ref.shape
    parts = d_ref.shape[0]
    tall = share // parts
    streams = [stacked(d_ref, at, tall) for at in range(3)]
    extra = [d_ref[q, 3 * tall : 3 * tall + 8, :].astype(f32) for q in range(parts)]
    row = row_ref[0:1, :]
    means, pulls, dots = [], [], []
    for at in range(2):
        means.append(jnp.sum(streams[at].astype(f32) * row, axis=1, keepdims=True) * (1.0 / width_all))
        dot = jnp.concatenate(
            [upright(joined(e[0:3, 128 * at : 128 * (at + 1)]), tall) for e in extra], axis=0
        )
        dots.append(level(dot / cols_ref[:, 6 + at : 7 + at], width))
        s = cols_ref[:, 3 * at + 2 : 3 * at + 3]
        pulls.append(s * s * dot)
    dots = [*spread(jnp.concatenate(dots, axis=0)), jnp.zeros((2, width), f32)]
    dots = jnp.concatenate(dots, axis=0).astype(bf16)
    for j in range(blocks):
        left = whole(token_refs, j, 0)
        for at in range(2):
            p = nn(streams[at], left)
            cent = w_ref[j][at].astype(f32) - cols_ref[:, 3 * at : 3 * at + 1]
            grad = cols_ref[:, 3 * at + 1 : 3 * at + 2] * (p - means[at]) - cent * pulls[at]
            grad_ref[j][at * share : (at + 1) * share, :] = grad.astype(bf16)
        grad_ref[j][2 * share : 3 * share, :] = nn(streams[2], whole(token_refs, j, 1)).astype(bf16)
        grad_ref[j][3 * share :, :] = dots


def spread(sums):
    return [p.astype(f32) for k in range(2) for p in pieces(sums[k : k + 1, :])]


def token_back(d_ref, w0_ref, w1_ref, w2_ref, w3_ref, *refs):
    token_refs = refs[:2]
    cols_ref, rows_ref, mine_ref, theirs_ref, sums_ref = refs[2:]
    w_ref = (w0_ref, w1_ref, w2_ref, w3_ref)
    blocks = len(w_ref)
    _, share, width = w0_ref.shape
    tall = share // d_ref.shape[0]
    streams = [stacked(d_ref, at, tall).T for at in range(2)]
    hidden = stacked(d_ref, 2, tall)
    half = mine_ref.shape[1]
    for j in range(blocks):
        back = 0.0
        for at in range(2):
            cent = w_ref[j][at].astype(f32) - cols_ref[:, 3 * at : 3 * at + 1]
            back = back + nn(streams[at], (cent * cols_ref[:, 3 * at + 1 : 3 * at + 2]).astype(bf16))
        mine_ref[j] = back[:half]
        p = nn(hidden, whole(token_refs, j, 1))
        cent = w_ref[j][2].astype(f32) - rows_ref[j, 0:1, :]
        summed = jnp.sum(p, axis=0, keepdims=True)
        crossed = jnp.sum(p * cent, axis=0, keepdims=True)
        zero = jnp.zeros((6, width), f32)
        sums = jnp.concatenate([summed, crossed, zero], axis=0)
        sums_ref[j] = sums
        sums = jnp.concatenate([*spread(sums), zero[0:2]], axis=0)
        theirs_ref[j] = jnp.concatenate([back[half:], sums], axis=0).astype(bf16)


def both_cores(mine_ref, theirs_ref, sums_ref, out_ref):
    blocks, half, _ = mine_ref.shape
    lines = out_ref.shape[0]
    rows = half // lines
    for j in range(blocks):
        other = theirs_ref[j, half : half + 8, :].astype(f32)
        total = sums_ref[j, 0:2, :] + jnp.concatenate([joined(other[0:3]), joined(other[3:6])], axis=0)
        extra = jnp.concatenate([*spread(total), other[6:8]], axis=0).astype(bf16)
        for k in range(lines):
            at = slice(k * rows, (k + 1) * rows)
            out_ref[k, j, 0:rows, :] = (mine_ref[j, at, :] + theirs_ref[j, at, :].astype(f32)).astype(bf16)
            out_ref[k, j, rows : rows + 8, :] = extra


def whole_column(place_ref, in_ref, out_ref):
    lines, blocks, high, _ = in_ref.shape
    cuts = out_ref.shape[0]
    rows = (high - 8) // cuts
    for j in range(blocks):
        lots = [in_ref[y, j].astype(f32) for y in range(lines)]
        back = sum(lot[0 : high - 8] for lot in lots)
        total = [sum(joined(lot[high - 8 + 3 * k : high - 5 + 3 * k]) for lot in lots) for k in range(2)]
        extra = [p.astype(f32) for t in total for p in pieces(t)[0:2]]
        for l in range(cuts):
            out_ref[l, lax.rem(place_ref[1] + blocks - j, blocks)] = jnp.concatenate(
                [back[l * rows : (l + 1) * rows], *extra], axis=0
            ).astype(bf16)


def finish_wide(place_ref, g0_ref, g1_ref, g2_ref, g3_ref, gate_ref, up_ref, store_ref):
    g_ref = (g0_ref, g1_ref, g2_ref, g3_ref)
    share = store_ref.shape[1]
    for at, ref in enumerate((gate_ref, up_ref)):
        for k, g in enumerate(g_ref):
            store_ref[lax.rem(place_ref[1] + k, len(g_ref))] = g[at * share : (at + 1) * share, :].astype(f32)
        ref[...] = store_ref[...].reshape(-1, store_ref.shape[2]).T


def finish_tall(
    hidden_all, place_ref, in_ref, cotangent_ref, g0_ref, g1_ref, g2_ref, g3_ref, down_ref, rows_ref, gain_ref,
    tokens_ref, grad_ref, dgain_ref, dots_ref,
):
    lines, blocks, _, width = in_ref.shape
    rows = tokens_ref.shape[0]
    lots = [in_ref[l, j].astype(f32) for l in range(lines) for j in range(blocks)]
    total = sum(lots)
    tokens_ref[...] = cotangent_ref[...].astype(f32) + total[0:rows]
    summed = total[rows : rows + 1] + total[rows + 1 : rows + 2]
    crossed = total[rows + 2 : rows + 3] + total[rows + 3 : rows + 4]
    mine = rows_ref[0]
    mean, scale = mine[0:1, :], mine[2:3, :]
    gain = gain_ref[...]
    dgain_ref[...] = scale * crossed
    g_ref = (g0_ref, g1_ref, g2_ref, g3_ref)
    share = down_ref.shape[1]
    for k, g in enumerate(g_ref):
        j = lax.rem(place_ref[1] + k, len(g_ref))
        dots = g[3 * share :, :].astype(f32)
        dots_ref[j] = jnp.concatenate([joined(dots[0:3]), joined(dots[3:6]), jnp.zeros((6, width), f32)], axis=0)
        cent = down_ref[j].astype(f32) - mean
        grad_ref[j] = scale * gain * (g[2 * share : 3 * share, :].astype(f32) - summed * (1.0 / hidden_all)) - (
            scale * scale * scale * gain * crossed
        ) * cent


def call(body, outs, *args, place=None, scratch=(), far=0, grant=20):
    specs = [pl.BlockSpec(memory_space=pltpu.HBM if i < far else pltpu.VMEM) for i in range(len(args))]
    if place is not None:
        args = (place, *args)
        specs = [pl.BlockSpec(memory_space=pltpu.SMEM), *specs]
    return pl.pallas_call(
        body,
        out_shape=[jax.ShapeDtypeStruct(s, t) for s, t in outs],
        in_specs=specs,
        scratch_shapes=scratch,
        compiler_params=pltpu.CompilerParams(vmem_limit_bytes=grant << 20),
    )(*args)


def exchange(x, axis):
    return lax.all_to_all(x, axis, split_axis=0, concat_axis=0, tiled=True)


def shift(x, axis, by):
    size = lax.axis_size(axis)
    return lax.ppermute(x, axis, [(i, (i + by) % size) for i in range(size)])


def apart(x, axis, by):
    size = lax.axis_size(axis)
    outer = axis in BLK

    def spot(core, i):
        return i % size * 2 + core if outer else core * size + i % size

    pairs = [(spot(core, i), spot(core, i + by * (1 - 2 * core))) for core in (0, 1) for i in range(size)]
    return lax.ppermute(x, (axis, "core") if outer else ("core", axis), pairs)


def block(tokens, cotangent, gate_weight, up_weight, down_weight, gate_gain, up_gain, down_gain):
    rows, width = tokens.shape
    hidden = gate_weight.shape[1]
    nx, nz, ny = lax.axis_size("x"), lax.axis_size("zh"), lax.axis_size("y")
    nl, nc = lax.axis_size("zl"), lax.axis_size("core")
    width_all = width * nx * nz
    hidden_all = hidden * ny * nl * nc
    share = hidden // nx
    tall = share // nz
    count = rows * ny * nl * nc
    place = jnp.stack(
        [lax.axis_index("zh"), lax.axis_index("x"), lax.axis_index("zl"), lax.axis_index("y"), lax.axis_index("core")]
    ).astype(jnp.int32)
    swap = [(0, 1), (1, 0)]

    def grid_exchange(x, axes):
        flat = exchange(x.reshape(x.shape[0] * x.shape[1], *x.shape[2:]), axes)
        return flat.reshape(x.shape)

    (both,) = call(
        pack_tokens, [((nx, nl, rows + 4, 2 * width), bf16)],
        down_weight, down_gain.reshape(1, width), tokens, cotangent,
        far=4,
        grant=60,
        scratch=[
            pltpu.VMEM((hidden, width), bf16), pltpu.VMEM((1, width), f32),
            pltpu.VMEM((rows, width), bf16), pltpu.VMEM((rows, width), bf16), pltpu.SemaphoreType.DMA((4,)),
        ],
    )
    both = grid_exchange(both, ("x", "zl"))
    cut_weights = call(
        pack_weights, [((3, share, width), bf16)] * nx, gate_weight, up_weight, down_weight,
        place=place,
        far=3,
        scratch=[
            pltpu.VMEM((nx, 3, share, width), bf16),
            pltpu.VMEM((width, hidden), bf16), pltpu.VMEM((width, hidden), bf16), pltpu.VMEM((hidden, width), bf16),
            pltpu.SemaphoreType.DMA((3,)),
        ],
    )
    weights = [cut_weights[0], None, None, None]
    for k in (2, 1, 3):
        weights[k] = shift(cut_weights[k], "x", k)
    (both,) = call(
        functools.partial(repack_tokens, hidden), [((ny, nx, nl * rows + 8, 2 * width), bf16)], both, place=place
    )
    own = exchange(both, "y")
    other = lax.ppermute(own, "core", swap)
    piece, sent = ((3 * tall, count), bf16), ((3 * tall + 8, count), bf16)
    kept, first, second, third, rows_of, news = call(
        functools.partial(forward, hidden * nl),
        [piece, sent, sent, piece, ((nx, 8, width), f32), ((8, count), bf16)],
        *weights, own, other,
        place=place,
        scratch=[pltpu.VMEM((nz, 3 * tall, count), bf16)],
    )
    first = apart(first, "zh", 1)
    second = apart(second, "zh", -1)
    (third,) = call(add_pair, [sent], third, first)
    third = apart(third, "zh", 1)
    d, cols, row = call(
        functools.partial(gating, width * nx),
        [((3 * tall + 8, count), bf16), ((share, 128), f32), ((8, count), f32)],
        kept, first, second, third, news, gate_gain.reshape(1, hidden), up_gain.reshape(1, hidden),
        place=place,
    )
    d = lax.all_gather(d, "zh")

    half = count // nc
    mine, theirs, sums = call(
        token_back, [((nx, half, width), f32), ((nx, half + 8, width), bf16), ((nx, 8, width), f32)],
        d, *weights, own, other, cols, rows_of,
    )
    theirs = lax.ppermute(theirs, "core", swap)
    grads = call(
        functools.partial(weight_grads, width_all), [((3 * share + 8, width), bf16)] * nx,
        d, *weights, own, other, cols, row,
    )
    (back,) = call(both_cores, [((ny, nx, nl * rows + 8, width), bf16)], mine, theirs, sums)
    back = exchange(back, "y")
    met = [grads[0], None, None, None]
    for k in (2, 1, 3):
        met[k] = shift(grads[k], "x", -k)
    (back,) = call(whole_column, [((nl, nx, rows + 4, width), bf16)], back, place=place)
    back = grid_exchange(back, ("zl", "x"))
    grad_gate, grad_up = call(finish_wide, [((width, hidden), f32), ((width, hidden), f32)], *met,
        place=place, scratch=[pltpu.VMEM((nx, share, width), f32)],
    )
    grad_tokens, grad_down, down_dgain, dots = call(
        functools.partial(finish_tall, hidden_all),
        [((rows, width), f32), ((nx, share, width), f32), ((1, width), f32), ((nx, 8, width), f32)],
        back, cotangent, *met, down_weight.reshape(nx, share, width), rows_of, down_gain.reshape(1, width),
        place=place,
    )
    return (
        grad_tokens,
        grad_gate,
        grad_up,
        grad_down.reshape(hidden, width),
        dots[:, 0, :share].reshape(hidden),
        dots[:, 1, :share].reshape(hidden),
        down_dgain.reshape(width),
    )


def solution(mesh):
    fine = Mesh(mesh.devices.reshape(4, 4, 2, 4, 4), (*BLK, *REP))
    return jax.shard_map(
        block,
        mesh=fine,
        in_specs=(
            P(BLK, REP), P(BLK, REP), P(REP, BLK), P(REP, BLK), P(BLK, REP), P(BLK), P(BLK), P(REP),
        ),
        out_specs=(
            P(BLK, REP), P(REP, BLK), P(REP, BLK), P(BLK, REP), P(BLK), P(BLK), P(REP),
        ),
        check_vma=False,
    )
```

```python
import functools

import jax
import jax.numpy as jnp
from jax import lax
from jax.experimental import pallas as pl
from jax.experimental.pallas import tpu as pltpu
from jax.sharding import Mesh, PartitionSpec as P


epsilon = 0.0001
branch_scale = 0.5
bf16 = jnp.bfloat16
f32 = jnp.float32

BLK = ("y", "zl", "core")
REP = ("zh", "x")


def nn(a, b):
    return lax.dot_general(a, b, (((1,), (0,)), ((), ())), preferred_element_type=f32)


def nt(a, b):
    return lax.dot_general(a, b, (((1,), (1,)), ((), ())), preferred_element_type=f32)


def pieces(x):
    high = x.astype(bf16)
    rest = x - high.astype(f32)
    middle = rest.astype(bf16)
    return high, middle, (rest - middle.astype(f32)).astype(bf16)


def joined(rows):
    return rows[0:1].astype(f32) + rows[1:2].astype(f32) + rows[2:3].astype(f32)


def merged(moments, count):
    mean = sum(m for m, _ in moments) * (1.0 / len(moments))
    square = sum(s for _, s in moments)
    for m, _ in moments:
        square = square + count * ((m - mean) * (m - mean))
    return mean, square


def upright(row, tall):
    shape = (tall, row.shape[1])
    same = lax.broadcasted_iota(jnp.int32, shape, 0) == lax.broadcasted_iota(jnp.int32, shape, 1)
    return jnp.sum(jnp.where(same, row, 0.0), axis=1, keepdims=True)


def level(col, wide):
    shape = (col.shape[0], wide)
    same = lax.broadcasted_iota(jnp.int32, shape, 0) == lax.broadcasted_iota(jnp.int32, shape, 1)
    return jnp.sum(jnp.where(same, col, 0.0), axis=0, keepdims=True)


def fetched(pairs, sems):
    copies = [pltpu.make_async_copy(a, b, sems.at[i]) for i, (a, b) in enumerate(pairs)]
    for c in copies:
        c.start()
    return copies


def pack_tokens(
    down_hbm, gain_hbm, tokens_hbm, cotangent_hbm, out_ref, down_ref, gain_ref, tokens_ref, cotangent_ref, sems
):
    copies = fetched(
        ((down_hbm, down_ref), (gain_hbm, gain_ref), (tokens_hbm, tokens_ref), (cotangent_hbm, cotangent_ref)), sems
    )
    _, width = tokens_ref.shape
    copies[0].wait()
    w = down_ref[...].astype(f32)
    mean = jnp.sum(w, axis=0, keepdims=True) * (1.0 / w.shape[0])
    off = w - mean
    square = jnp.sum(off * off, axis=0, keepdims=True)
    for c in copies[1:]:
        c.wait()
    scaled = (branch_scale * cotangent_ref[...].astype(f32)).astype(bf16)
    gain = pieces(gain_ref[...])
    left = [tokens_ref[...], *pieces(mean), gain[0]]
    right = [scaled, *pieces(square), gain[1]]
    for side, parts in enumerate((left, right)):
        block = jnp.concatenate([p.astype(f32) for p in parts], axis=0).astype(bf16)
        for j in range(out_ref.shape[0]):
            for l in range(out_ref.shape[1]):
                out_ref[j, l, :, side * width : (side + 1) * width] = block


def pack_weights(place_ref, gate_hbm, up_hbm, down_hbm, *refs):
    *outs, store_ref, gate_ref, up_ref, down_ref, sems = refs
    copies = fetched(((gate_hbm, gate_ref), (up_hbm, up_ref), (down_hbm, down_ref)), sems)
    blocks, _, share, _ = store_ref.shape
    for at, ref in enumerate((gate_ref, up_ref)):
        copies[at].wait()
        turned = ref[...].astype(f32).T.astype(bf16)
        for j in range(blocks):
            store_ref[j, at] = turned[j * share : (j + 1) * share]
    copies[2].wait()
    for j in range(blocks):
        store_ref[j, 2] = down_ref[j * share : (j + 1) * share]
    for k in range(blocks):
        outs[k][...] = store_ref[lax.rem(place_ref[1] + k, blocks)]


def repack_tokens(tall_count, place_ref, in_ref, out_ref):
    blocks, lines, high, wide = in_ref.shape
    rows = high - 4
    width = wide // 2
    for j in range(blocks):
        source = lax.rem(place_ref[1] + blocks - j, blocks)
        lots = [in_ref[source, l, 0 : rows + 4, :].astype(f32) for l in range(lines)]
        moments = [
            (joined(lot[rows : rows + 3, 0:width]), joined(lot[rows : rows + 3, width:])) for lot in lots
        ]
        mean, square = merged(moments, tall_count)
        zero = jnp.zeros((4, width), f32)
        for extra, a in ((mean, 0), (square, width)):
            parts = [lot[0:rows, a : a + width] for lot in lots]
            parts += [p.astype(f32) for p in pieces(extra)]
            parts += [lots[0][rows + 3 : rows + 4, a : a + width], zero]
            block = jnp.concatenate(parts, axis=0).astype(bf16)
            for y in range(out_ref.shape[0]):
                out_ref[y, j, :, a : a + width] = block


def whole(token_refs, j, at):
    rows = token_refs[0].shape[2] - 8
    width = token_refs[0].shape[3] // 2
    halves = [ref[:, j, 0:rows, at * width : (at + 1) * width].reshape(-1, width) for ref in token_refs]
    return jnp.concatenate(halves, axis=0)


def moments_of(w_ref, at):
    blocks = [w[at].astype(f32) for w in w_ref]
    mean = sum(jnp.sum(w, axis=1, keepdims=True) for w in blocks) * (1.0 / (len(blocks) * blocks[0].shape[1]))
    square = sum(jnp.sum((w - mean) * (w - mean), axis=1, keepdims=True) for w in blocks)
    return mean, square


def weight_moments(w0_ref, w1_ref, w2_ref, w3_ref, mean_ref, line_ref):
    lane = lax.broadcasted_iota(jnp.int32, mean_ref.shape, 1)
    means = jnp.zeros(mean_ref.shape, f32)
    for at in range(2):
        mean, square = moments_of((w0_ref, w1_ref, w2_ref, w3_ref), at)
        means = jnp.where(lane == at, mean, means)
        width = line_ref.shape[1] // 2
        line_ref[at : at + 1, 0:width] = level(mean, width)
        line_ref[at : at + 1, width : 2 * width] = level(square, width)
    mean_ref[...] = means


def forward(
    tall_count, place_ref, w0_ref, w1_ref, w2_ref, w3_ref, *refs
):
    token_refs = refs[:2]
    mean_ref, line_ref = refs[2:4]
    kept_ref, first_ref, second_ref, third_ref, rows_ref, news_ref, store_ref = refs[4:]
    w_ref = (w0_ref, w1_ref, w2_ref, w3_ref)
    blocks = len(w_ref)
    _, share, width = w0_ref.shape
    parts = store_ref.shape[0]
    tall = share // parts
    lefts = [whole(token_refs, j, 0) for j in range(blocks)]
    ones = jnp.ones((8, width), bf16)
    row = sum(nt(ones, left) for left in lefts)[0:1]
    for at in range(2):
        mean = mean_ref[:, at : at + 1]
        total = sum(nt(w_ref[j][at], lefts[j]) for j in range(blocks))
        total = (total - mean * row).astype(bf16)
        for q in range(parts):
            store_ref[q, at * tall : (at + 1) * tall, :] = total[q * tall : (q + 1) * tall]
    rest = jnp.zeros((1, row.shape[1] - 512), f32)
    lines = [row] + [jnp.concatenate([line_ref[at : at + 1, :], rest], axis=1) for at in range(2)]
    lines = [p.astype(f32) for line in lines for p in pieces(line)[0:2]]
    news_ref[...] = jnp.concatenate([*lines, jnp.zeros((2, row.shape[1]), f32)], axis=0).astype(bf16)
    total = 0.0
    rows = token_refs[0].shape[2] - 8
    for j in range(blocks):
        lots = [
            ref[y, j, rows : rows + 8, :].astype(f32) for ref in token_refs for y in range(token_refs[0].shape[0])
        ]
        mean, square = merged([(joined(lot[:, 0:width]), joined(lot[:, width:])) for lot in lots], tall_count)
        scale = lax.rsqrt(square + epsilon)
        gain = lots[0][3:4, 0:width] + lots[0][3:4, width:]
        gs = gain * scale
        rows_ref[j] = jnp.concatenate([mean, gs, scale, jnp.zeros((5, width), f32)], axis=0)
        hat = ((w_ref[j][2].astype(f32) - mean) * gs).astype(bf16)
        total = total + nt(hat, whole(token_refs, j, 1))
    total = total.astype(bf16)
    for q in range(parts):
        store_ref[q, 2 * tall : 3 * tall, :] = total[q * tall : (q + 1) * tall]
    at, core = place_ref[0], place_ref[4]
    for ref, k in ((kept_ref, 0), (first_ref, 2), (second_ref, 3 - 2 * core), (third_ref, 1 + 2 * core)):
        ref[0 : 3 * tall, :] = store_ref[lax.rem(at + k, parts)]
    for ref in (first_ref, second_ref):
        ref[3 * tall : 3 * tall + 8, :] = news_ref[...]


def add_pair(a_ref, b_ref, out_ref):
    high = a_ref.shape[0]
    out_ref[0:high, :] = (a_ref[...].astype(f32) + b_ref[0:high, :].astype(f32)).astype(bf16)
    out_ref[high:, :] = b_ref[high:, :]


def gating(
    wide_count, place_ref, kept_ref, first_ref, second_ref, third_ref, news_ref, gate_gain_ref, up_gain_ref,
    d_ref, cols_ref, row_ref,
):
    tall = (d_ref.shape[0] - 8) // 3
    share = cols_ref.shape[0]
    high = 3 * tall
    news = [news_ref[...].astype(f32)]
    news += [ref[high : high + 8, :].astype(f32) for ref in (first_ref, second_ref, third_ref)]
    rows = [n[0:1] + n[1:2] for n in news]
    row = sum(rows)
    row_ref[...] = jnp.broadcast_to(row, row_ref.shape)
    wide = 256
    lines = [None] * 16
    for at in range(2):
        both = [n[2 * at + 2 : 2 * at + 3] + n[2 * at + 3 : 2 * at + 4] for n in news]
        moments = [(b[:, 0:wide], b[:, wide : 2 * wide]) for b in both]
        mean, square = merged(moments, wide_count)
        gains = (gate_gain_ref, up_gain_ref)[at]
        gain = sum(
            jnp.where(place_ref[1] == j, gains[:, j * share : (j + 1) * share], 0.0)
            for j in range(gains.shape[1] // share)
        )
        gain = jnp.concatenate([gain, jnp.zeros((1, wide - share), f32)], axis=1)
        scale = lax.rsqrt(square + epsilon)
        lines[3 * at : 3 * at + 3] = [mean, gain * scale, scale]
        lines[6 + at] = gain
        lines[8 + 4 * at : 12 + 4 * at] = [m for m, _ in moments]
    lines.append(jnp.zeros((cols_ref.shape[1] - 16, wide), f32))
    cols_ref[...] = jnp.concatenate(lines, axis=0).T[0:share]
    mine = cols_ref[pl.ds(pl.multiple_of(place_ref[0] * tall, 8), tall), :]
    total = kept_ref[...].astype(f32) + second_ref[0:high, :].astype(f32) + third_ref[0:high, :].astype(f32)
    sums = []
    for at in range(2):
        x = total[at * tall : (at + 1) * tall] - mine[:, 3 * at : 3 * at + 1] * row
        for q, r in enumerate(rows):
            x = x + mine[:, 8 + 4 * at + q : 9 + 4 * at + q] * r
        sums.append(mine[:, 3 * at + 1 : 3 * at + 2] * x)
    gate, up = sums
    dhidden = total[2 * tall : 3 * tall]
    sig = 1.0 / (1.0 + jnp.exp(-gate))
    act = gate * sig
    d_gate = (dhidden * up * sig * (1.0 + gate * (1.0 - sig))).astype(bf16)
    d_up = (dhidden * act).astype(bf16)
    d_ref[2 * tall : 3 * tall, :] = (act * up).astype(bf16)
    d_ref[0:tall, :] = d_gate
    d_ref[tall : 2 * tall, :] = d_up
    dots = [
        level(jnp.sum(d.astype(f32) * v, axis=1, keepdims=True), 128)
        for d, v in ((d_gate, gate), (d_up, up))
    ]
    wide = d_ref.shape[1]
    dots = jnp.concatenate([*dots, jnp.zeros((1, wide - 256), f32)], axis=1)
    extra = [p.astype(f32) for p in pieces(dots)] + [jnp.zeros((5, wide), f32)]
    d_ref[3 * tall : 3 * tall + 8, :] = jnp.concatenate(extra, axis=0).astype(bf16)


def stacked(d_ref, at, tall):
    return jnp.concatenate(
        [d_ref[q, at * tall : (at + 1) * tall, :] for q in range(d_ref.shape[0])], axis=0
    )


def weight_grads(width_all, d_ref, w0_ref, w1_ref, w2_ref, w3_ref, *refs):
    token_refs = refs[:2]
    cols_ref, row_ref, *grad_ref = refs[2:]
    w_ref = (w0_ref, w1_ref, w2_ref, w3_ref)
    blocks = len(w_ref)
    _, share, width = w0_ref.shape
    parts = d_ref.shape[0]
    tall = share // parts
    streams = [stacked(d_ref, at, tall) for at in range(3)]
    extra = [d_ref[q, 3 * tall : 3 * tall + 8, :].astype(f32) for q in range(parts)]
    row = row_ref[0:1, :]
    means, pulls, dots = [], [], []
    for at in range(2):
        means.append(jnp.sum(streams[at].astype(f32) * row, axis=1, keepdims=True) * (1.0 / width_all))
        dot = jnp.concatenate(
            [upright(joined(e[0:3, 128 * at : 128 * (at + 1)]), tall) for e in extra], axis=0
        )
        dots.append(level(dot / cols_ref[:, 6 + at : 7 + at], width))
        s = cols_ref[:, 3 * at + 2 : 3 * at + 3]
        pulls.append(s * s * dot)
    dots = [*spread(jnp.concatenate(dots, axis=0)), jnp.zeros((2, width), f32)]
    dots = jnp.concatenate(dots, axis=0).astype(bf16)
    for j in range(blocks):
        left = whole(token_refs, j, 0)
        for at in range(2):
            p = nn(streams[at], left)
            cent = w_ref[j][at].astype(f32) - cols_ref[:, 3 * at : 3 * at + 1]
            grad = cols_ref[:, 3 * at + 1 : 3 * at + 2] * (p - means[at]) - cent * pulls[at]
            grad_ref[j][at * share : (at + 1) * share, :] = grad.astype(bf16)
        grad_ref[j][2 * share : 3 * share, :] = nn(streams[2], whole(token_refs, j, 1)).astype(bf16)
        grad_ref[j][3 * share :, :] = dots


def spread(sums):
    return [p.astype(f32) for k in range(2) for p in pieces(sums[k : k + 1, :])]


def token_back(d_ref, w0_ref, w1_ref, w2_ref, w3_ref, *refs):
    token_refs = refs[:2]
    cols_ref, rows_ref, mine_ref, theirs_ref, sums_ref = refs[2:]
    w_ref = (w0_ref, w1_ref, w2_ref, w3_ref)
    blocks = len(w_ref)
    _, share, width = w0_ref.shape
    tall = share // d_ref.shape[0]
    streams = [stacked(d_ref, at, tall).T for at in range(2)]
    hidden = stacked(d_ref, 2, tall)
    half = mine_ref.shape[1]
    for j in range(blocks):
        back = 0.0
        for at in range(2):
            cent = w_ref[j][at].astype(f32) - cols_ref[:, 3 * at : 3 * at + 1]
            back = back + nn(streams[at], (cent * cols_ref[:, 3 * at + 1 : 3 * at + 2]).astype(bf16))
        mine_ref[j] = back[:half]
        p = nn(hidden, whole(token_refs, j, 1))
        cent = w_ref[j][2].astype(f32) - rows_ref[j, 0:1, :]
        summed = jnp.sum(p, axis=0, keepdims=True)
        crossed = jnp.sum(p * cent, axis=0, keepdims=True)
        zero = jnp.zeros((6, width), f32)
        sums = jnp.concatenate([summed, crossed, zero], axis=0)
        sums_ref[j] = sums
        sums = jnp.concatenate([*spread(sums), zero[0:2]], axis=0)
        theirs_ref[j] = jnp.concatenate([back[half:], sums], axis=0).astype(bf16)


def both_cores(mine_ref, theirs_ref, sums_ref, out_ref):
    blocks, half, _ = mine_ref.shape
    lines = out_ref.shape[0]
    rows = half // lines
    for j in range(blocks):
        other = theirs_ref[j, half : half + 8, :].astype(f32)
        total = sums_ref[j, 0:2, :] + jnp.concatenate([joined(other[0:3]), joined(other[3:6])], axis=0)
        extra = jnp.concatenate([*spread(total), other[6:8]], axis=0).astype(bf16)
        for k in range(lines):
            at = slice(k * rows, (k + 1) * rows)
            out_ref[k, j, 0:rows, :] = (mine_ref[j, at, :] + theirs_ref[j, at, :].astype(f32)).astype(bf16)
            out_ref[k, j, rows : rows + 8, :] = extra


def whole_column(place_ref, in_ref, out_ref):
    lines, blocks, high, _ = in_ref.shape
    cuts = out_ref.shape[0]
    rows = (high - 8) // cuts
    for j in range(blocks):
        lots = [in_ref[y, j].astype(f32) for y in range(lines)]
        back = sum(lot[0 : high - 8] for lot in lots)
        total = [sum(joined(lot[high - 8 + 3 * k : high - 5 + 3 * k]) for lot in lots) for k in range(2)]
        extra = [p.astype(f32) for t in total for p in pieces(t)[0:2]]
        for l in range(cuts):
            out_ref[l, lax.rem(place_ref[1] + blocks - j, blocks)] = jnp.concatenate(
                [back[l * rows : (l + 1) * rows], *extra], axis=0
            ).astype(bf16)


def finish_wide(place_ref, g0_ref, g1_ref, g2_ref, g3_ref, gate_ref, up_ref, store_ref):
    g_ref = (g0_ref, g1_ref, g2_ref, g3_ref)
    share = store_ref.shape[1]
    for at, ref in enumerate((gate_ref, up_ref)):
        for k, g in enumerate(g_ref):
            store_ref[lax.rem(place_ref[1] + k, len(g_ref))] = g[at * share : (at + 1) * share, :].astype(f32)
        ref[...] = store_ref[...].reshape(-1, store_ref.shape[2]).T


def finish_tall(
    hidden_all, place_ref, in_ref, cotangent_ref, g0_ref, g1_ref, g2_ref, g3_ref, down_ref, rows_ref, gain_ref,
    tokens_ref, grad_ref, dgain_ref, dots_ref,
):
    lines, blocks, _, width = in_ref.shape
    rows = tokens_ref.shape[0]
    lots = [in_ref[l, j].astype(f32) for l in range(lines) for j in range(blocks)]
    total = sum(lots)
    tokens_ref[...] = cotangent_ref[...].astype(f32) + total[0:rows]
    summed = total[rows : rows + 1] + total[rows + 1 : rows + 2]
    crossed = total[rows + 2 : rows + 3] + total[rows + 3 : rows + 4]
    mine = rows_ref[0]
    mean, scale = mine[0:1, :], mine[2:3, :]
    gain = gain_ref[...]
    dgain_ref[...] = scale * crossed
    g_ref = (g0_ref, g1_ref, g2_ref, g3_ref)
    share = down_ref.shape[1]
    for k, g in enumerate(g_ref):
        j = lax.rem(place_ref[1] + k, len(g_ref))
        dots = g[3 * share :, :].astype(f32)
        dots_ref[j] = jnp.concatenate([joined(dots[0:3]), joined(dots[3:6]), jnp.zeros((6, width), f32)], axis=0)
        cent = down_ref[j].astype(f32) - mean
        grad_ref[j] = scale * gain * (g[2 * share : 3 * share, :].astype(f32) - summed * (1.0 / hidden_all)) - (
            scale * scale * scale * gain * crossed
        ) * cent


def call(body, outs, *args, place=None, scratch=(), far=0, grant=20):
    specs = [pl.BlockSpec(memory_space=pltpu.HBM if i < far else pltpu.VMEM) for i in range(len(args))]
    if place is not None:
        args = (place, *args)
        specs = [pl.BlockSpec(memory_space=pltpu.SMEM), *specs]
    return pl.pallas_call(
        body,
        out_shape=[jax.ShapeDtypeStruct(s, t) for s, t in outs],
        in_specs=specs,
        scratch_shapes=scratch,
        compiler_params=pltpu.CompilerParams(vmem_limit_bytes=grant << 20),
    )(*args)


def exchange(x, axis):
    return lax.all_to_all(x, axis, split_axis=0, concat_axis=0, tiled=True)


def shift(x, axis, by):
    size = lax.axis_size(axis)
    return lax.ppermute(x, axis, [(i, (i + by) % size) for i in range(size)])


def apart(x, axis, by):
    size = lax.axis_size(axis)
    outer = axis in BLK

    def spot(core, i):
        return i % size * 2 + core if outer else core * size + i % size

    pairs = [(spot(core, i), spot(core, i + by * (1 - 2 * core))) for core in (0, 1) for i in range(size)]
    return lax.ppermute(x, (axis, "core") if outer else ("core", axis), pairs)


def block(tokens, cotangent, gate_weight, up_weight, down_weight, gate_gain, up_gain, down_gain):
    rows, width = tokens.shape
    hidden = gate_weight.shape[1]
    nx, nz, ny = lax.axis_size("x"), lax.axis_size("zh"), lax.axis_size("y")
    nl, nc = lax.axis_size("zl"), lax.axis_size("core")
    width_all = width * nx * nz
    hidden_all = hidden * ny * nl * nc
    share = hidden // nx
    tall = share // nz
    count = rows * ny * nl * nc
    place = jnp.stack(
        [lax.axis_index("zh"), lax.axis_index("x"), lax.axis_index("zl"), lax.axis_index("y"), lax.axis_index("core")]
    ).astype(jnp.int32)
    swap = [(0, 1), (1, 0)]

    def grid_exchange(x, axes):
        flat = exchange(x.reshape(x.shape[0] * x.shape[1], *x.shape[2:]), axes)
        return flat.reshape(x.shape)

    (both,) = call(
        pack_tokens, [((nx, nl, rows + 4, 2 * width), bf16)],
        down_weight, down_gain.reshape(1, width), tokens, cotangent,
        far=4,
        grant=60,
        scratch=[
            pltpu.VMEM((hidden, width), bf16), pltpu.VMEM((1, width), f32),
            pltpu.VMEM((rows, width), bf16), pltpu.VMEM((rows, width), bf16), pltpu.SemaphoreType.DMA((4,)),
        ],
    )
    both = grid_exchange(both, ("x", "zl"))
    cut_weights = call(
        pack_weights, [((3, share, width), bf16)] * nx, gate_weight, up_weight, down_weight,
        place=place,
        far=3,
        scratch=[
            pltpu.VMEM((nx, 3, share, width), bf16),
            pltpu.VMEM((width, hidden), bf16), pltpu.VMEM((width, hidden), bf16), pltpu.VMEM((hidden, width), bf16),
            pltpu.SemaphoreType.DMA((3,)),
        ],
    )
    weights = [cut_weights[0], None, None, None]
    for k in (2, 1, 3):
        weights[k] = shift(cut_weights[k], "x", k)
    (both,) = call(
        functools.partial(repack_tokens, hidden), [((ny, nx, nl * rows + 8, 2 * width), bf16)], both, place=place
    )
    own = exchange(both, "y")
    other = lax.ppermute(own, "core", swap)
    means, lines = call(weight_moments, [((share, 128), f32), ((2, 512), f32)], *weights)
    piece, sent = ((3 * tall, count), bf16), ((3 * tall + 8, count), bf16)
    kept, first, second, third, rows_of, news = call(
        functools.partial(forward, hidden * nl),
        [piece, sent, sent, piece, ((nx, 8, width), f32), ((8, count), bf16)],
        *weights, own, other, means, lines,
        place=place,
        scratch=[pltpu.VMEM((nz, 3 * tall, count), bf16)],
    )
    first = apart(first, "zh", 1)
    second = apart(second, "zh", -1)
    (third,) = call(add_pair, [sent], third, first)
    third = apart(third, "zh", 1)
    d, cols, row = call(
        functools.partial(gating, width * nx),
        [((3 * tall + 8, count), bf16), ((share, 128), f32), ((8, count), f32)],
        kept, first, second, third, news, gate_gain.reshape(1, hidden), up_gain.reshape(1, hidden),
        place=place,
    )
    d = lax.all_gather(d, "zh")

    half = count // nc
    mine, theirs, sums = call(
        token_back, [((nx, half, width), f32), ((nx, half + 8, width), bf16), ((nx, 8, width), f32)],
        d, *weights, own, other, cols, rows_of,
    )
    theirs = lax.ppermute(theirs, "core", swap)
    grads = call(
        functools.partial(weight_grads, width_all), [((3 * share + 8, width), bf16)] * nx,
        d, *weights, own, other, cols, row,
    )
    (back,) = call(both_cores, [((ny, nx, nl * rows + 8, width), bf16)], mine, theirs, sums)
    back = exchange(back, "y")
    met = [grads[0], None, None, None]
    for k in (2, 1, 3):
        met[k] = shift(grads[k], "x", -k)
    (back,) = call(whole_column, [((nl, nx, rows + 4, width), bf16)], back, place=place)
    back = grid_exchange(back, ("zl", "x"))
    grad_gate, grad_up = call(finish_wide, [((width, hidden), f32), ((width, hidden), f32)], *met,
        place=place, scratch=[pltpu.VMEM((nx, share, width), f32)],
    )
    grad_tokens, grad_down, down_dgain, dots = call(
        functools.partial(finish_tall, hidden_all),
        [((rows, width), f32), ((nx, share, width), f32), ((1, width), f32), ((nx, 8, width), f32)],
        back, cotangent, *met, down_weight.reshape(nx, share, width), rows_of, down_gain.reshape(1, width),
        place=place,
    )
    return (
        grad_tokens,
        grad_gate,
        grad_up,
        grad_down.reshape(hidden, width),
        dots[:, 0, :share].reshape(hidden),
        dots[:, 1, :share].reshape(hidden),
        down_dgain.reshape(width),
    )


def solution(mesh):
    fine = Mesh(mesh.devices.reshape(4, 4, 2, 4, 4), (*BLK, *REP))
    return jax.shard_map(
        block,
        mesh=fine,
        in_specs=(
            P(BLK, REP), P(BLK, REP), P(REP, BLK), P(REP, BLK), P(BLK, REP), P(BLK), P(BLK), P(REP),
        ),
        out_specs=(
            P(BLK, REP), P(REP, BLK), P(REP, BLK), P(BLK, REP), P(BLK), P(BLK), P(REP),
        ),
        check_vma=False,
    )
```

```python
import functools

import jax
import jax.numpy as jnp
from jax import lax
from jax.experimental import pallas as pl
from jax.experimental.pallas import tpu as pltpu
from jax.sharding import Mesh, PartitionSpec as P


epsilon = 0.0001
branch_scale = 0.5
bf16 = jnp.bfloat16
f32 = jnp.float32

BLK = ("y", "zl", "core")
REP = ("zh", "x")


def nn(a, b):
    return lax.dot_general(a, b, (((1,), (0,)), ((), ())), preferred_element_type=f32)


def nt(a, b):
    return lax.dot_general(a, b, (((1,), (1,)), ((), ())), preferred_element_type=f32)


def pieces(x):
    high = x.astype(bf16)
    rest = x - high.astype(f32)
    middle = rest.astype(bf16)
    return high, middle, (rest - middle.astype(f32)).astype(bf16)


def joined(rows):
    return rows[0:1].astype(f32) + rows[1:2].astype(f32) + rows[2:3].astype(f32)


def merged(moments, count):
    mean = sum(m for m, _ in moments) * (1.0 / len(moments))
    square = sum(s for _, s in moments)
    for m, _ in moments:
        square = square + count * ((m - mean) * (m - mean))
    return mean, square


def upright(row, tall):
    shape = (tall, row.shape[1])
    same = lax.broadcasted_iota(jnp.int32, shape, 0) == lax.broadcasted_iota(jnp.int32, shape, 1)
    return jnp.sum(jnp.where(same, row, 0.0), axis=1, keepdims=True)


def level(col, wide):
    shape = (col.shape[0], wide)
    same = lax.broadcasted_iota(jnp.int32, shape, 0) == lax.broadcasted_iota(jnp.int32, shape, 1)
    return jnp.sum(jnp.where(same, col, 0.0), axis=0, keepdims=True)


def fetched(pairs, sems):
    copies = [pltpu.make_async_copy(a, b, sems.at[i]) for i, (a, b) in enumerate(pairs)]
    for c in copies:
        c.start()
    return copies


def pack_tokens(
    down_hbm, gain_hbm, tokens_hbm, cotangent_hbm, out_ref, down_ref, gain_ref, tokens_ref, cotangent_ref, sems
):
    cuts = sems.shape[0] - 3
    high = down_ref.shape[0] // cuts
    spans = [slice(i * high, (i + 1) * high) for i in range(cuts)]
    copies = fetched(
        [
            *((down_hbm.at[at], down_ref.at[at]) for at in spans),
            (gain_hbm, gain_ref), (tokens_hbm, tokens_ref), (cotangent_hbm, cotangent_ref),
        ],
        sems,
    )
    _, width = tokens_ref.shape
    moments = []
    for c, at in zip(copies, spans):
        c.wait()
        w = down_ref[at, :].astype(f32)
        mean = jnp.sum(w, axis=0, keepdims=True) * (1.0 / high)
        off = w - mean
        moments.append((mean, jnp.sum(off * off, axis=0, keepdims=True)))
    mean, square = merged(moments, high)
    for c in copies[cuts:]:
        c.wait()
    scaled = (branch_scale * cotangent_ref[...].astype(f32)).astype(bf16)
    gain = pieces(gain_ref[...])
    left = [tokens_ref[...], *pieces(mean), gain[0]]
    right = [scaled, *pieces(square), gain[1]]
    for side, parts in enumerate((left, right)):
        block = jnp.concatenate([p.astype(f32) for p in parts], axis=0).astype(bf16)
        for j in range(out_ref.shape[0]):
            for l in range(out_ref.shape[1]):
                out_ref[j, l, :, side * width : (side + 1) * width] = block


def pack_weights(place_ref, gate_hbm, up_hbm, down_hbm, *refs):
    *outs, store_ref, gate_ref, up_ref, down_ref, sems = refs
    copies = fetched(((gate_hbm, gate_ref), (up_hbm, up_ref), (down_hbm, down_ref)), sems)
    blocks, _, share, _ = store_ref.shape
    for at, ref in enumerate((gate_ref, up_ref)):
        copies[at].wait()
        turned = ref[...].astype(f32).T.astype(bf16)
        for j in range(blocks):
            store_ref[j, at] = turned[j * share : (j + 1) * share]
    copies[2].wait()
    for j in range(blocks):
        store_ref[j, 2] = down_ref[j * share : (j + 1) * share]
    for k in range(blocks):
        outs[k][...] = store_ref[lax.rem(place_ref[1] + k, blocks)]


def repack_tokens(tall_count, place_ref, in_ref, out_ref):
    blocks, lines, high, wide = in_ref.shape
    rows = high - 4
    width = wide // 2
    for j in range(blocks):
        source = lax.rem(place_ref[1] + blocks - j, blocks)
        lots = [in_ref[source, l, 0 : rows + 4, :].astype(f32) for l in range(lines)]
        moments = [
            (joined(lot[rows : rows + 3, 0:width]), joined(lot[rows : rows + 3, width:])) for lot in lots
        ]
        mean, square = merged(moments, tall_count)
        zero = jnp.zeros((4, width), f32)
        for extra, a in ((mean, 0), (square, width)):
            parts = [lot[0:rows, a : a + width] for lot in lots]
            parts += [p.astype(f32) for p in pieces(extra)]
            parts += [lots[0][rows + 3 : rows + 4, a : a + width], zero]
            block = jnp.concatenate(parts, axis=0).astype(bf16)
            for y in range(out_ref.shape[0]):
                out_ref[y, j, :, a : a + width] = block


def whole(token_refs, j, at):
    rows = token_refs[0].shape[2] - 8
    width = token_refs[0].shape[3] // 2
    halves = [ref[:, j, 0:rows, at * width : (at + 1) * width].reshape(-1, width) for ref in token_refs]
    return jnp.concatenate(halves, axis=0)


def moments_of(w_ref, at):
    blocks = [w[at].astype(f32) for w in w_ref]
    mean = sum(jnp.sum(w, axis=1, keepdims=True) for w in blocks) * (1.0 / (len(blocks) * blocks[0].shape[1]))
    square = sum(jnp.sum((w - mean) * (w - mean), axis=1, keepdims=True) for w in blocks)
    return mean, square


def weight_moments(w0_ref, w1_ref, w2_ref, w3_ref, mean_ref, line_ref):
    lane = lax.broadcasted_iota(jnp.int32, mean_ref.shape, 1)
    means = jnp.zeros(mean_ref.shape, f32)
    for at in range(2):
        mean, square = moments_of((w0_ref, w1_ref, w2_ref, w3_ref), at)
        means = jnp.where(lane == at, mean, means)
        width = line_ref.shape[1] // 2
        line_ref[at : at + 1, 0:width] = level(mean, width)
        line_ref[at : at + 1, width : 2 * width] = level(square, width)
    mean_ref[...] = means


def forward(
    tall_count, place_ref, w0_ref, w1_ref, w2_ref, w3_ref, *refs
):
    token_refs = refs[:2]
    mean_ref, line_ref = refs[2:4]
    kept_ref, first_ref, second_ref, third_ref, rows_ref, news_ref, store_ref = refs[4:]
    w_ref = (w0_ref, w1_ref, w2_ref, w3_ref)
    blocks = len(w_ref)
    _, share, width = w0_ref.shape
    parts = store_ref.shape[0]
    tall = share // parts
    lefts = [whole(token_refs, j, 0) for j in range(blocks)]
    ones = jnp.ones((8, width), bf16)
    row = sum(nt(ones, left) for left in lefts)[0:1]
    for at in range(2):
        mean = mean_ref[:, at : at + 1]
        total = sum(nt(w_ref[j][at], lefts[j]) for j in range(blocks))
        total = (total - mean * row).astype(bf16)
        for q in range(parts):
            store_ref[q, at * tall : (at + 1) * tall, :] = total[q * tall : (q + 1) * tall]
    rest = jnp.zeros((1, row.shape[1] - 512), f32)
    lines = [row] + [jnp.concatenate([line_ref[at : at + 1, :], rest], axis=1) for at in range(2)]
    lines = [p.astype(f32) for line in lines for p in pieces(line)[0:2]]
    news_ref[...] = jnp.concatenate([*lines, jnp.zeros((2, row.shape[1]), f32)], axis=0).astype(bf16)
    total = 0.0
    rows = token_refs[0].shape[2] - 8
    for j in range(blocks):
        lots = [
            ref[y, j, rows : rows + 8, :].astype(f32) for ref in token_refs for y in range(token_refs[0].shape[0])
        ]
        mean, square = merged([(joined(lot[:, 0:width]), joined(lot[:, width:])) for lot in lots], tall_count)
        scale = lax.rsqrt(square + epsilon)
        gain = lots[0][3:4, 0:width] + lots[0][3:4, width:]
        gs = gain * scale
        rows_ref[j] = jnp.concatenate([mean, gs, scale, jnp.zeros((5, width), f32)], axis=0)
        hat = ((w_ref[j][2].astype(f32) - mean) * gs).astype(bf16)
        total = total + nt(hat, whole(token_refs, j, 1))
    total = total.astype(bf16)
    for q in range(parts):
        store_ref[q, 2 * tall : 3 * tall, :] = total[q * tall : (q + 1) * tall]
    at, core = place_ref[0], place_ref[4]
    for ref, k in ((kept_ref, 0), (first_ref, 2), (second_ref, 3 - 2 * core), (third_ref, 1 + 2 * core)):
        ref[0 : 3 * tall, :] = store_ref[lax.rem(at + k, parts)]
    for ref in (first_ref, second_ref):
        ref[3 * tall : 3 * tall + 8, :] = news_ref[...]


def add_pair(a_ref, b_ref, out_ref):
    high = a_ref.shape[0]
    out_ref[0:high, :] = (a_ref[...].astype(f32) + b_ref[0:high, :].astype(f32)).astype(bf16)
    out_ref[high:, :] = b_ref[high:, :]


def gating(
    wide_count, place_ref, kept_ref, first_ref, second_ref, third_ref, news_ref, gate_gain_ref, up_gain_ref,
    d_ref, cols_ref, row_ref,
):
    tall = (d_ref.shape[0] - 8) // 3
    share = cols_ref.shape[0]
    high = 3 * tall
    news = [news_ref[...].astype(f32)]
    news += [ref[high : high + 8, :].astype(f32) for ref in (first_ref, second_ref, third_ref)]
    rows = [n[0:1] + n[1:2] for n in news]
    row = sum(rows)
    row_ref[...] = jnp.broadcast_to(row, row_ref.shape)
    wide = 256
    lines = [None] * 16
    for at in range(2):
        both = [n[2 * at + 2 : 2 * at + 3] + n[2 * at + 3 : 2 * at + 4] for n in news]
        moments = [(b[:, 0:wide], b[:, wide : 2 * wide]) for b in both]
        mean, square = merged(moments, wide_count)
        gains = (gate_gain_ref, up_gain_ref)[at]
        gain = sum(
            jnp.where(place_ref[1] == j, gains[:, j * share : (j + 1) * share], 0.0)
            for j in range(gains.shape[1] // share)
        )
        gain = jnp.concatenate([gain, jnp.zeros((1, wide - share), f32)], axis=1)
        scale = lax.rsqrt(square + epsilon)
        lines[3 * at : 3 * at + 3] = [mean, gain * scale, scale]
        lines[6 + at] = gain
        lines[8 + 4 * at : 12 + 4 * at] = [m for m, _ in moments]
    lines.append(jnp.zeros((cols_ref.shape[1] - 16, wide), f32))
    cols_ref[...] = jnp.concatenate(lines, axis=0).T[0:share]
    mine = cols_ref[pl.ds(pl.multiple_of(place_ref[0] * tall, 8), tall), :]
    total = kept_ref[...].astype(f32) + second_ref[0:high, :].astype(f32) + third_ref[0:high, :].astype(f32)
    sums = []
    for at in range(2):
        x = total[at * tall : (at + 1) * tall] - mine[:, 3 * at : 3 * at + 1] * row
        for q, r in enumerate(rows):
            x = x + mine[:, 8 + 4 * at + q : 9 + 4 * at + q] * r
        sums.append(mine[:, 3 * at + 1 : 3 * at + 2] * x)
    gate, up = sums
    dhidden = total[2 * tall : 3 * tall]
    sig = 1.0 / (1.0 + jnp.exp(-gate))
    act = gate * sig
    d_gate = (dhidden * up * sig * (1.0 + gate * (1.0 - sig))).astype(bf16)
    d_up = (dhidden * act).astype(bf16)
    d_ref[2 * tall : 3 * tall, :] = (act * up).astype(bf16)
    d_ref[0:tall, :] = d_gate
    d_ref[tall : 2 * tall, :] = d_up
    dots = [
        level(jnp.sum(d.astype(f32) * v, axis=1, keepdims=True), 128)
        for d, v in ((d_gate, gate), (d_up, up))
    ]
    wide = d_ref.shape[1]
    dots = jnp.concatenate([*dots, jnp.zeros((1, wide - 256), f32)], axis=1)
    extra = [p.astype(f32) for p in pieces(dots)] + [jnp.zeros((5, wide), f32)]
    d_ref[3 * tall : 3 * tall + 8, :] = jnp.concatenate(extra, axis=0).astype(bf16)


def stacked(d_ref, at, tall):
    return jnp.concatenate(
        [d_ref[q, at * tall : (at + 1) * tall, :] for q in range(d_ref.shape[0])], axis=0
    )


def weight_grads(width_all, d_ref, w0_ref, w1_ref, w2_ref, w3_ref, *refs):
    token_refs = refs[:2]
    cols_ref, row_ref, *grad_ref = refs[2:]
    w_ref = (w0_ref, w1_ref, w2_ref, w3_ref)
    blocks = len(w_ref)
    _, share, width = w0_ref.shape
    parts = d_ref.shape[0]
    tall = share // parts
    streams = [stacked(d_ref, at, tall) for at in range(3)]
    extra = [d_ref[q, 3 * tall : 3 * tall + 8, :].astype(f32) for q in range(parts)]
    row = row_ref[0:1, :]
    means, pulls, dots = [], [], []
    for at in range(2):
        means.append(jnp.sum(streams[at].astype(f32) * row, axis=1, keepdims=True) * (1.0 / width_all))
        dot = jnp.concatenate(
            [upright(joined(e[0:3, 128 * at : 128 * (at + 1)]), tall) for e in extra], axis=0
        )
        dots.append(level(dot / cols_ref[:, 6 + at : 7 + at], width))
        s = cols_ref[:, 3 * at + 2 : 3 * at + 3]
        pulls.append(s * s * dot)
    dots = [*spread(jnp.concatenate(dots, axis=0)), jnp.zeros((2, width), f32)]
    dots = jnp.concatenate(dots, axis=0).astype(bf16)
    for j in range(blocks):
        left = whole(token_refs, j, 0)
        for at in range(2):
            p = nn(streams[at], left)
            cent = w_ref[j][at].astype(f32) - cols_ref[:, 3 * at : 3 * at + 1]
            grad = cols_ref[:, 3 * at + 1 : 3 * at + 2] * (p - means[at]) - cent * pulls[at]
            grad_ref[j][at * share : (at + 1) * share, :] = grad.astype(bf16)
        grad_ref[j][2 * share : 3 * share, :] = nn(streams[2], whole(token_refs, j, 1)).astype(bf16)
        grad_ref[j][3 * share :, :] = dots


def spread(sums):
    return [p.astype(f32) for k in range(2) for p in pieces(sums[k : k + 1, :])]


def token_back(d_ref, w0_ref, w1_ref, w2_ref, w3_ref, *refs):
    token_refs = refs[:2]
    cols_ref, rows_ref, mine_ref, theirs_ref, sums_ref = refs[2:]
    w_ref = (w0_ref, w1_ref, w2_ref, w3_ref)
    blocks = len(w_ref)
    _, share, width = w0_ref.shape
    tall = share // d_ref.shape[0]
    streams = [stacked(d_ref, at, tall).T for at in range(2)]
    hidden = stacked(d_ref, 2, tall)
    half = mine_ref.shape[1]
    for j in range(blocks):
        back = 0.0
        for at in range(2):
            cent = w_ref[j][at].astype(f32) - cols_ref[:, 3 * at : 3 * at + 1]
            back = back + nn(streams[at], (cent * cols_ref[:, 3 * at + 1 : 3 * at + 2]).astype(bf16))
        mine_ref[j] = back[:half]
        p = nn(hidden, whole(token_refs, j, 1))
        cent = w_ref[j][2].astype(f32) - rows_ref[j, 0:1, :]
        summed = jnp.sum(p, axis=0, keepdims=True)
        crossed = jnp.sum(p * cent, axis=0, keepdims=True)
        zero = jnp.zeros((6, width), f32)
        sums = jnp.concatenate([summed, crossed, zero], axis=0)
        sums_ref[j] = sums
        sums = jnp.concatenate([*spread(sums), zero[0:2]], axis=0)
        theirs_ref[j] = jnp.concatenate([back[half:], sums], axis=0).astype(bf16)


def both_cores(mine_ref, theirs_ref, sums_ref, out_ref):
    blocks, half, _ = mine_ref.shape
    lines = out_ref.shape[0]
    rows = half // lines
    for j in range(blocks):
        other = theirs_ref[j, half : half + 8, :].astype(f32)
        total = sums_ref[j, 0:2, :] + jnp.concatenate([joined(other[0:3]), joined(other[3:6])], axis=0)
        extra = jnp.concatenate([*spread(total), other[6:8]], axis=0).astype(bf16)
        for k in range(lines):
            at = slice(k * rows, (k + 1) * rows)
            out_ref[k, j, 0:rows, :] = (mine_ref[j, at, :] + theirs_ref[j, at, :].astype(f32)).astype(bf16)
            out_ref[k, j, rows : rows + 8, :] = extra


def whole_column(place_ref, in_ref, out_ref):
    lines, blocks, high, _ = in_ref.shape
    cuts = out_ref.shape[0]
    rows = (high - 8) // cuts
    for j in range(blocks):
        lots = [in_ref[y, j].astype(f32) for y in range(lines)]
        back = sum(lot[0 : high - 8] for lot in lots)
        total = [sum(joined(lot[high - 8 + 3 * k : high - 5 + 3 * k]) for lot in lots) for k in range(2)]
        extra = [p.astype(f32) for t in total for p in pieces(t)[0:2]]
        for l in range(cuts):
            out_ref[l, lax.rem(place_ref[1] + blocks - j, blocks)] = jnp.concatenate(
                [back[l * rows : (l + 1) * rows], *extra], axis=0
            ).astype(bf16)


def finish_wide(place_ref, g0_ref, g1_ref, g2_ref, g3_ref, gate_ref, up_ref, store_ref):
    g_ref = (g0_ref, g1_ref, g2_ref, g3_ref)
    share = store_ref.shape[1]
    for at, ref in enumerate((gate_ref, up_ref)):
        for k, g in enumerate(g_ref):
            store_ref[lax.rem(place_ref[1] + k, len(g_ref))] = g[at * share : (at + 1) * share, :].astype(f32)
        ref[...] = store_ref[...].reshape(-1, store_ref.shape[2]).T


def finish_tall(
    hidden_all, place_ref, in_ref, cotangent_ref, g0_ref, g1_ref, g2_ref, g3_ref, down_ref, rows_ref, gain_ref,
    tokens_ref, grad_ref, dgain_ref, dots_ref,
):
    lines, blocks, _, width = in_ref.shape
    rows = tokens_ref.shape[0]
    lots = [in_ref[l, j].astype(f32) for l in range(lines) for j in range(blocks)]
    total = sum(lots)
    tokens_ref[...] = cotangent_ref[...].astype(f32) + total[0:rows]
    summed = total[rows : rows + 1] + total[rows + 1 : rows + 2]
    crossed = total[rows + 2 : rows + 3] + total[rows + 3 : rows + 4]
    mine = rows_ref[0]
    mean, scale = mine[0:1, :], mine[2:3, :]
    gain = gain_ref[...]
    dgain_ref[...] = scale * crossed
    g_ref = (g0_ref, g1_ref, g2_ref, g3_ref)
    share = down_ref.shape[1]
    for k, g in enumerate(g_ref):
        j = lax.rem(place_ref[1] + k, len(g_ref))
        dots = g[3 * share :, :].astype(f32)
        dots_ref[j] = jnp.concatenate([joined(dots[0:3]), joined(dots[3:6]), jnp.zeros((6, width), f32)], axis=0)
        cent = down_ref[j].astype(f32) - mean
        grad_ref[j] = scale * gain * (g[2 * share : 3 * share, :].astype(f32) - summed * (1.0 / hidden_all)) - (
            scale * scale * scale * gain * crossed
        ) * cent


def call(body, outs, *args, place=None, scratch=(), far=0, grant=20):
    specs = [pl.BlockSpec(memory_space=pltpu.HBM if i < far else pltpu.VMEM) for i in range(len(args))]
    if place is not None:
        args = (place, *args)
        specs = [pl.BlockSpec(memory_space=pltpu.SMEM), *specs]
    return pl.pallas_call(
        body,
        out_shape=[jax.ShapeDtypeStruct(s, t) for s, t in outs],
        in_specs=specs,
        scratch_shapes=scratch,
        compiler_params=pltpu.CompilerParams(vmem_limit_bytes=grant << 20),
    )(*args)


def exchange(x, axis):
    return lax.all_to_all(x, axis, split_axis=0, concat_axis=0, tiled=True)


def shift(x, axis, by):
    size = lax.axis_size(axis)
    return lax.ppermute(x, axis, [(i, (i + by) % size) for i in range(size)])


def apart(x, axis, by):
    size = lax.axis_size(axis)
    outer = axis in BLK

    def spot(core, i):
        return i % size * 2 + core if outer else core * size + i % size

    pairs = [(spot(core, i), spot(core, i + by * (1 - 2 * core))) for core in (0, 1) for i in range(size)]
    return lax.ppermute(x, (axis, "core") if outer else ("core", axis), pairs)


def block(tokens, cotangent, gate_weight, up_weight, down_weight, gate_gain, up_gain, down_gain):
    rows, width = tokens.shape
    hidden = gate_weight.shape[1]
    nx, nz, ny = lax.axis_size("x"), lax.axis_size("zh"), lax.axis_size("y")
    nl, nc = lax.axis_size("zl"), lax.axis_size("core")
    width_all = width * nx * nz
    hidden_all = hidden * ny * nl * nc
    share = hidden // nx
    tall = share // nz
    count = rows * ny * nl * nc
    place = jnp.stack(
        [lax.axis_index("zh"), lax.axis_index("x"), lax.axis_index("zl"), lax.axis_index("y"), lax.axis_index("core")]
    ).astype(jnp.int32)
    swap = [(0, 1), (1, 0)]

    def grid_exchange(x, axes):
        flat = exchange(x.reshape(x.shape[0] * x.shape[1], *x.shape[2:]), axes)
        return flat.reshape(x.shape)

    (both,) = call(
        pack_tokens, [((nx, nl, rows + 4, 2 * width), bf16)],
        down_weight, down_gain.reshape(1, width), tokens, cotangent,
        far=4,
        grant=60,
        scratch=[
            pltpu.VMEM((hidden, width), bf16), pltpu.VMEM((1, width), f32),
            pltpu.VMEM((rows, width), bf16), pltpu.VMEM((rows, width), bf16), pltpu.SemaphoreType.DMA((7,)),
        ],
    )
    both = grid_exchange(both, ("x", "zl"))
    cut_weights = call(
        pack_weights, [((3, share, width), bf16)] * nx, gate_weight, up_weight, down_weight,
        place=place,
        far=3,
        scratch=[
            pltpu.VMEM((nx, 3, share, width), bf16),
            pltpu.VMEM((width, hidden), bf16), pltpu.VMEM((width, hidden), bf16), pltpu.VMEM((hidden, width), bf16),
            pltpu.SemaphoreType.DMA((3,)),
        ],
    )
    weights = [cut_weights[0], None, None, None]
    for k in (2, 1, 3):
        weights[k] = shift(cut_weights[k], "x", k)
    (both,) = call(
        functools.partial(repack_tokens, hidden), [((ny, nx, nl * rows + 8, 2 * width), bf16)], both, place=place
    )
    own = exchange(both, "y")
    other = lax.ppermute(own, "core", swap)
    means, lines = call(weight_moments, [((share, 128), f32), ((2, 512), f32)], *weights)
    piece, sent = ((3 * tall, count), bf16), ((3 * tall + 8, count), bf16)
    kept, first, second, third, rows_of, news = call(
        functools.partial(forward, hidden * nl),
        [piece, sent, sent, piece, ((nx, 8, width), f32), ((8, count), bf16)],
        *weights, own, other, means, lines,
        place=place,
        scratch=[pltpu.VMEM((nz, 3 * tall, count), bf16)],
    )
    first = apart(first, "zh", 1)
    second = apart(second, "zh", -1)
    (third,) = call(add_pair, [sent], third, first)
    third = apart(third, "zh", 1)
    d, cols, row = call(
        functools.partial(gating, width * nx),
        [((3 * tall + 8, count), bf16), ((share, 128), f32), ((8, count), f32)],
        kept, first, second, third, news, gate_gain.reshape(1, hidden), up_gain.reshape(1, hidden),
        place=place,
    )
    d = lax.all_gather(d, "zh")

    half = count // nc
    mine, theirs, sums = call(
        token_back, [((nx, half, width), f32), ((nx, half + 8, width), bf16), ((nx, 8, width), f32)],
        d, *weights, own, other, cols, rows_of,
    )
    theirs = lax.ppermute(theirs, "core", swap)
    grads = call(
        functools.partial(weight_grads, width_all), [((3 * share + 8, width), bf16)] * nx,
        d, *weights, own, other, cols, row,
    )
    (back,) = call(both_cores, [((ny, nx, nl * rows + 8, width), bf16)], mine, theirs, sums)
    back = exchange(back, "y")
    met = [grads[0], None, None, None]
    for k in (2, 1, 3):
        met[k] = shift(grads[k], "x", -k)
    (back,) = call(whole_column, [((nl, nx, rows + 4, width), bf16)], back, place=place)
    back = grid_exchange(back, ("zl", "x"))
    grad_gate, grad_up = call(finish_wide, [((width, hidden), f32), ((width, hidden), f32)], *met,
        place=place, scratch=[pltpu.VMEM((nx, share, width), f32)],
    )
    grad_tokens, grad_down, down_dgain, dots = call(
        functools.partial(finish_tall, hidden_all),
        [((rows, width), f32), ((nx, share, width), f32), ((1, width), f32), ((nx, 8, width), f32)],
        back, cotangent, *met, down_weight.reshape(nx, share, width), rows_of, down_gain.reshape(1, width),
        place=place,
    )
    return (
        grad_tokens,
        grad_gate,
        grad_up,
        grad_down.reshape(hidden, width),
        dots[:, 0, :share].reshape(hidden),
        dots[:, 1, :share].reshape(hidden),
        down_dgain.reshape(width),
    )


def solution(mesh):
    fine = Mesh(mesh.devices.reshape(4, 4, 2, 4, 4), (*BLK, *REP))
    return jax.shard_map(
        block,
        mesh=fine,
        in_specs=(
            P(BLK, REP), P(BLK, REP), P(REP, BLK), P(REP, BLK), P(BLK, REP), P(BLK), P(BLK), P(REP),
        ),
        out_specs=(
            P(BLK, REP), P(REP, BLK), P(REP, BLK), P(BLK, REP), P(BLK), P(BLK), P(REP),
        ),
        check_vma=False,
    )
```
